32 devices in a mesh: pop: 8 (over z, x), mp: 4 (over y, core).
Axes of the slice: x: 2, y: 2, z: 4, core: 2. Of those that a mesh axis runs over, the one named last changes fastest.
Arguments:
- tokens: bfloat16 [256, 3584], replicated, may hold values from -60 to 60
- target: bfloat16 [256, 3584], P(None, 'mp'), may hold values from -6 to 6
- w_query: bfloat16 [3584, 3584], P('pop', 'mp'), may hold values from -0.09375 to 0.09375
- w_key: bfloat16 [3584, 512], P(None, 'mp'), may hold values from -0.09375 to 0.09375
- w_value: bfloat16 [3584, 512], P(None, 'mp'), may hold values from -0.09375 to 0.09375
- w_out: bfloat16 [3584, 3584], P('mp', 'pop'), may hold values from -0.09375 to 0.09375
- query_left_factors: bfloat16 [8, 3584, 4], P('pop'), may hold values from -0.09375 to 0.09375
- query_right_factors: bfloat16 [8, 4, 3584], P('pop', None, 'mp'), may hold values from -6 to 6
- o_left: bfloat16 [8, 3584, 4], P('pop', 'mp'), may hold values from -0.09375 to 0.09375
- o_right: bfloat16 [8, 4, 3584], P('pop'), may hold values from -6 to 6
- member_ids: int32 [8], P('pop'), may hold values from 0 to 7, each once
Outputs:
- grad_query: float32 [3584, 3584], P('pop', 'mp')
- grad_out: float32 [3584, 3584], P('mp', 'pop')
- fitness: float32 [8], P('pop')
The draws below stay inside these ranges and needn't reach their ends.
Inputs may be any that keep to these rules, and one draw needn't show every extreme that they name: `member_ids`: every number from 0 to 7 appears once.
All inputs are finite; a program needn't handle non-finite values.
Results may differ from the reference program's by a relative error of at most 0.005.
Values may be sent and summed in bfloat16 or wider, within the bound.
A program may use at most 64 MiB of HBM per device.

```python
import math
import jax
import jax.numpy as jnp
from jax import lax

D = 3584
HEADS = 28
KV_HEADS = 4
HEAD_DIM = 128
RANK = 4
TOK = 256
F = 3584
KVF = 512
M = 8
N_MP = 4


def draw_tokens(key, part):
    first = jax.random.fold_in(key, 0)
    normal = jax.random.normal(first, (TOK, D), jnp.float32)
    return jnp.clip(normal, -5.0, 5.0).astype(jnp.bfloat16)


def level_of(stream_key, dims, cuts, low, largest):
    def one(axis_at, parts):
        draws = jax.random.uniform(jax.random.fold_in(jax.random.fold_in(stream_key, 6), axis_at), (parts,), jnp.float32, low / len(cuts), largest / len(cuts))
        return jnp.repeat(jnp.exp(draws), dims[axis_at] // parts).reshape((-1,) + (1,) * (len(dims) - axis_at - 1))

    gain = one(*cuts[0])
    for cut in cuts[1:]:
        gain = gain * one(*cut)
    return gain


def normal_values(stream_key, shape, scale, bound, shards=(), held_as=jnp.bfloat16):
    result = scale * jax.random.normal(stream_key, shape, jnp.float32)
    if shards:
        result = result * level_of(stream_key, shape, shards, -0.22, 0.18)
    return jnp.clip(result, -bound, bound).astype(held_as)


def setup_inputs(seed: int = 0) -> dict:
    key_list = jax.random.split(jax.random.key(seed), 12)
    return {
        "tokens": draw_tokens(jax.random.fold_in(key_list[11], 71), 0),
        "target": normal_values(key_list[1], (TOK, D), 1.0, 6.0, ((1, 4),)),
        "w_query": normal_values(key_list[2], (D, F), D ** -0.5, 0.09375, ((0, 8), (1, 4))),
        "w_key": normal_values(key_list[3], (D, KVF), D ** -0.5, 0.09375, ((1, 4),)),
        "w_value": normal_values(key_list[4], (D, KVF), D ** -0.5, 0.09375, ((1, 4),)),
        "w_out": normal_values(key_list[5], (F, D), F ** -0.5, 0.09375, ((0, 4), (1, 8))),
        "query_left_factors": normal_values(key_list[6], (M, D, RANK), D ** -0.5, 0.09375, ((0, 8),)),
        "query_right_factors": normal_values(key_list[7], (M, RANK, F), 1.0, 6.0, ((0, 8), (2, 4))),
        "o_left": normal_values(key_list[8], (M, F, RANK), F ** -0.5, 0.09375, ((0, 8), (1, 4))),
        "o_right": normal_values(key_list[9], (M, RANK, D), 1.0, 6.0, ((0, 8),)),
        "member_ids": jax.random.permutation(key_list[10], M).astype(jnp.int32),
    }


noise_scale = 0.5
rope_base = 1000000.0
spread_floor = 0.001

def tables(count, head_size):
    position = jnp.arange(count, dtype=jnp.float32)
    index = jnp.arange(head_size // 2, dtype=jnp.float32)
    freq = jnp.exp(-math.log(rope_base) * 2.0 * index / head_size)
    angle = position[:, None] * freq[None, :]
    return (jnp.cos(angle)[:, None, :], jnp.sin(angle)[:, None, :])

def rotate(field, cosine_table, sine):
    half = field.shape[-1] // 2
    first = field[..., :half]
    second = field[..., half:]
    return jnp.concatenate([first * cosine_table - second * sine, second * cosine_table + first * sine], axis=-1)

def reference(tokens, target, w_query, w_key, w_value, w_out, query_left_factors, query_right_factors, o_left, o_right, member_ids):
    tok = tokens.shape[0]
    width = tokens.shape[1]
    hidden = w_query.shape[1]
    members = query_left_factors.shape[0]
    group = HEADS // KV_HEADS
    block = hidden // N_MP
    scale = HEAD_DIM ** (-0.5)
    cosine_table, sine = tables(tok, HEAD_DIM)
    base = jnp.dot(tokens, w_query, preferred_element_type=jnp.float32)
    keys = rotate(jnp.dot(tokens, w_key, preferred_element_type=jnp.float32).reshape(tok, KV_HEADS, HEAD_DIM), cosine_table, sine).astype(jnp.bfloat16)
    values = jnp.dot(tokens, w_value, preferred_element_type=jnp.float32).astype(jnp.bfloat16).reshape(tok, KV_HEADS, HEAD_DIM)
    signs = (1 - 2 * (member_ids % 2)).astype(jnp.float32)
    causal = jnp.arange(tok)[:, None] >= jnp.arange(tok)[None, :]
    target_f = target.astype(jnp.float32)

    def score(index):
        sign = signs[index]
        lowrank_product = jnp.dot(tokens, query_left_factors[index], preferred_element_type=jnp.float32).astype(jnp.bfloat16)
        query = base + noise_scale * sign * jnp.dot(lowrank_product, query_right_factors[index], preferred_element_type=jnp.float32)
        query = rotate(query.reshape(tok, HEADS, HEAD_DIM), cosine_table, sine).astype(jnp.bfloat16)
        query = query.reshape(tok, KV_HEADS, group, HEAD_DIM)
        scores = jnp.einsum('tkgd,skd->kgts', query.astype(jnp.float32), keys.astype(jnp.float32)) * scale
        scores = jnp.where(causal, scores, -1e+30)
        probs = jax.nn.softmax(scores, axis=-1).astype(jnp.bfloat16)
        mixed = jnp.einsum('kgts,skd->tkgd', probs.astype(jnp.float32), values.astype(jnp.float32)).astype(jnp.bfloat16).reshape(tok, hidden)
        total = jnp.zeros((tok, width), jnp.float32)
        for part in range(N_MP):
            rows = mixed[:, part * block:(part + 1) * block]
            low_out = jnp.dot(rows, o_left[index, part * block:(part + 1) * block], preferred_element_type=jnp.float32)
            term = jnp.dot(rows, w_out[part * block:(part + 1) * block], preferred_element_type=jnp.float32)
            term = term + noise_scale * sign * jnp.dot(low_out, o_right[index].astype(jnp.float32), precision=lax.Precision.HIGHEST)
            rounded = lax.optimization_barrier(term.astype(jnp.bfloat16))
            total = total + rounded.astype(jnp.float32)
        diff = total - target_f
        return -(jnp.sum(diff * diff) / (tok * width))
    fitness = lax.map(score, jnp.arange(members))
    mean = jnp.sum(fitness) / members
    spread = jnp.sum((fitness - mean) * (fitness - mean)) / members
    weight = signs * (fitness - mean) / jnp.sqrt(spread + spread_floor)
    left_q = jnp.transpose(query_left_factors.astype(jnp.float32) * weight[:, None, None], (1, 0, 2)).reshape(width, members * RANK)
    right_q = query_right_factors.astype(jnp.float32).reshape(members * RANK, hidden)
    grad_query = jnp.dot(left_q, right_q, precision=lax.Precision.HIGHEST) / noise_scale
    output_left_factor = jnp.transpose(o_left.astype(jnp.float32) * weight[:, None, None], (1, 0, 2)).reshape(hidden, members * RANK)
    right_o = o_right.astype(jnp.float32).reshape(members * RANK, width)
    grad_out = jnp.dot(output_left_factor, right_o, precision=lax.Precision.HIGHEST) / noise_scale
    return (grad_query, grad_out, fitness)
```

```python
import functools
import math

import jax
import jax.numpy as jnp
import numpy as np
from jax import lax
from jax.experimental import pallas as pl
from jax.experimental.pallas import tpu as pltpu
from jax.sharding import PartitionSpec as P

HEAD_DIM = 128
RANK = 4
PACK = 8
LINK = jnp.bfloat16

noise_scale = 0.5
rope_base = 1000000.0
spread_floor = 0.001
MESH = pl.DeviceIdType.MESH
f32 = jnp.float32
bf16 = jnp.bfloat16


def rope_tables(count, head_size):
    index = np.arange(head_size // 2, dtype=np.float64)
    freq = np.exp(-math.log(rope_base) * 2.0 * index / head_size)
    angle = np.arange(count, dtype=np.float64)[:, None] * freq[None, :]
    cosine, sine = np.cos(angle), np.sin(angle)
    return (
        np.concatenate([cosine, cosine], 1).astype(np.float32),
        np.concatenate([-sine, sine], 1).astype(np.float32),
    )


def dot(a, b, dims=((1,), (0,))):
    return lax.dot_general(a, b, (dims, ((), ())), preferred_element_type=f32)


def split3(x):
    hi = x.astype(bf16)
    rest = x - hi.astype(f32)
    mid = rest.astype(bf16)
    low = (rest - mid.astype(f32)).astype(bf16)
    return hi, mid, low


def forward_kernel(
    n_pop, n_mp, width,
    tok_hbm, wq_hbm, wk_hbm, wv_hbm, wo_hbm, tgt_hbm, ql_ref, qr_ref, ol_ref, or_ref, id_ref,
    cos_ref, sin_ref, cos_rows, sin_rows,
    pack_a_out, pack_b_out, stat_out,
    tok_ref, wq_ref, kv_ref, wo_ref, tgt_ref,
    part_a, part_b, parts_a, parts_b, mine_l, packs_l, mine_q, packs_q, mine_o, packs_o,
    mine_b, packs_b, ring_a, ring_b,
    keys, values, low_rows, goal, mixed, terms, near_in, far_out, far_in, own_sum, total, errs,
    load_sem,
    pop_send, pop_recv,
    ring_send, ring_recv, near_send, near_recv, far_send, far_recv, err_send, err_recv,
):
    me = lax.axis_index("pop")
    mc = lax.axis_index("mp")
    n_dev = n_pop * n_mp
    tok, feats = tok_ref.shape[0], wq_ref.shape[1]
    cut = ring_a.shape[2]
    own_tok = tok // n_pop
    rows = n_pop * own_tok
    heads = feats // HEAD_DIM
    cols = wq_ref.shape[0]
    ranks = n_pop * RANK
    quarter = cols // n_mp
    odd = lax.rem(me, 2) == 1

    loads = [
        pltpu.make_async_copy(src, dst, load_sem.at[i])
        for i, (src, dst) in enumerate((
            (tok_hbm, tok_ref), (wq_hbm, wq_ref),
            (wk_hbm, kv_ref.at[:, :HEAD_DIM]), (wv_hbm, kv_ref.at[:, HEAD_DIM:]),
            (tgt_hbm, tgt_ref), (wo_hbm, wo_ref.at[:cols]),
        ))
    ]
    for load in loads:
        load.start()

    barrier = pltpu.get_barrier_semaphore()

    def greet(i, carry):
        other = lax.rem(mc * n_pop + me + i, n_dev)
        pl.semaphore_signal(
            barrier, inc=1,
            device_id={"pop": lax.rem(other, n_pop), "mp": other // n_pop},
            device_id_type=MESH,
        )
        return carry

    lax.fori_loop(1, n_dev, greet, 0)

    sign = 1 - 2 * lax.rem(id_ref[0], 2)
    factor = noise_scale * sign.astype(f32)
    loads[0].wait()
    loads[1].wait()
    window = tok_ref[:, pl.ds(pl.multiple_of(me // 2 * 2 * cols, 128), 2 * cols)]
    wq = wq_ref[...]
    first, second = window[:, :cols], window[:, cols:]
    base = dot(jnp.where(odd, second, first), wq)
    part_a[...] = base[:, :cut].reshape(part_a.shape).astype(LINK)
    part_b[...] = base[:, cut:].reshape(part_b.shape).astype(LINK)
    mine_q[...] = (qr_ref[...].astype(f32) * factor).astype(bf16)

    pl.semaphore_wait(barrier, n_dev - 1)

    def to_pop(i, kind):
        other = lax.rem(me + i, n_pop)
        src, dst = (
            (part_a.at[other], parts_a),
            (mine_q, packs_q),
            (mine_l, packs_l),
            (part_b.at[other], parts_b),
            (mine_o, packs_o),
            (mine_b.at[other], packs_b),
        )[kind]
        return pltpu.make_async_remote_copy(
            src_ref=src, dst_ref=dst.at[me], send_sem=pop_send.at[kind, i],
            recv_sem=pop_recv.at[kind, i], device_id={"pop": other}, device_id_type=MESH,
        )

    def to_all(kind):
        for i in range(1, n_pop):
            to_pop(i, kind).start()

    def from_all(kind):
        for i in range(1, n_pop):
            to_pop(i, kind).wait_recv()

    to_all(0)
    to_all(1)
    ql = ql_ref[...]
    mine_l[...] = dot(ql, tok_ref[...], ((1,), (1,))).astype(bf16)
    to_all(2)
    to_all(3)
    mine_o[...] = ol_ref[...]
    both = jnp.concatenate([ql.astype(f32), or_ref[...].astype(f32) * factor], axis=0)
    for q in range(n_pop):
        mine_b[q] = both[:, q * cols:(q + 1) * cols].astype(bf16)
    to_all(4)
    to_all(5)
    for mine, packs in ((part_a, parts_a), (part_b, parts_b), (mine_b, packs_b)):
        packs[me] = mine[me]
    packs_l[me] = mine_l[...]
    packs_q[me] = mine_q[...]
    packs_o[me] = mine_o[...]

    loads[2].wait()
    loads[3].wait()
    pair = dot(tok_ref[...], kv_ref[...])
    key = pair[:, :HEAD_DIM]
    key = (key * cos_ref[...] + pltpu.roll(key, HEAD_DIM // 2, 1) * sin_ref[...]).astype(bf16)
    values[:HEAD_DIM] = pair[:, HEAD_DIM:].T.astype(bf16)
    values[HEAD_DIM:] = jnp.ones((values.shape[0] - HEAD_DIM, tok), bf16)
    spot = lax.broadcasted_iota(jnp.int32, (tok, HEAD_DIM), 0)
    lane = lax.broadcasted_iota(jnp.int32, (tok, HEAD_DIM), 1)
    for q in range(n_pop):
        keys[q, :, :HEAD_DIM] = key
        hidden = (spot > q * own_tok + lane) & (lane < own_tok)
        keys[q, :, HEAD_DIM:] = jnp.where(hidden, -1e30, 0.0).astype(bf16)

    loads[4].wait()
    owner = me // (n_pop // n_mp)
    tgt = jnp.where(odd, tgt_ref[:, cols:], tgt_ref[:, :cols])
    goal[...] = jnp.where(mc == owner, -tgt, jnp.zeros_like(tgt))

    row_tok = lax.rem(lax.broadcasted_iota(jnp.int32, (own_tok, rows), 1), own_tok)
    pick_tok = (row_tok == lax.broadcasted_iota(jnp.int32, (own_tok, rows), 0)).astype(bf16)
    row_member = lax.broadcasted_iota(jnp.int32, (ranks, rows), 1) // own_tok
    same = row_member == lax.broadcasted_iota(jnp.int32, (ranks, rows), 0) // RANK

    def stacked(parts, *more):
        return jnp.concatenate(
            [p[i].astype(f32) for i in range(n_pop) for p in (parts,) + more], axis=0
        ).astype(bf16)

    from_all(1)
    from_all(2)
    pack_q = stacked(packs_q)
    low_all = stacked(packs_l)
    spot = lax.broadcasted_iota(jnp.int32, (tok, rows), 0)
    at_tok = lax.rem(lax.broadcasted_iota(jnp.int32, (tok, rows), 1), own_tok)
    for q in range(n_pop):
        sel = (spot == at_tok + q * own_tok).astype(bf16)
        low_rows[q] = jnp.where(same, dot(low_all, sel), 0.0).astype(bf16)

    def pop_at(r):
        r = lax.rem(r + 2 * n_pop, n_pop)
        return jnp.where(r < n_pop // 2, 2 * r, 2 * (n_pop - 1 - r) + 1)

    my_r = jnp.where(odd, n_pop - 1 - me // 2, me // 2)
    right, left = pop_at(my_r + 1), pop_at(my_r - 1)

    depth = n_pop // 2
    rings = (ring_a, ring_b)

    def hop(direction, step, g):
        at = pop_at(my_r - step if direction == 0 else my_r + step)
        return pltpu.make_async_remote_copy(
            src_ref=rings[g].at[at], dst_ref=rings[g].at[at],
            send_sem=ring_send.at[direction, step, g], recv_sem=ring_recv.at[direction, step, g],
            device_id={"pop": right if direction == 0 else left}, device_id_type=MESH,
        )

    def hops(direction, step, g):
        return step < depth - 1 or (step == depth - 1 and g == direction)

    for g, (kind, parts) in enumerate(((0, parts_a), (3, parts_b))):
        from_all(kind)
        sum_g = parts[0].astype(f32)
        for i in range(1, n_pop):
            sum_g = sum_g + parts[i].astype(f32)
        rings[g][me] = sum_g.astype(LINK)
        for direction in range(2):
            hop(direction, 0, g).start()

    from_all(4)
    from_all(5)
    pack_a_out[...] = stacked(packs_q, packs_o)
    pack_b_out[...] = stacked(packs_b)
    right_o = jnp.concatenate(
        [packs_b[i, RANK:].astype(f32) for i in range(n_pop)], axis=0
    ).astype(bf16)
    loads[5].wait()
    wo_ref[cols:] = stacked(packs_o)
    total[...] = jnp.zeros_like(total)

    scale = HEAD_DIM ** (-0.5) * math.log2(math.e)
    half = HEAD_DIM // 2
    filler = jnp.zeros((keys.shape[2] - HEAD_DIM - own_tok, rows), bf16)

    def attend(at):
        cosine = jnp.concatenate([cos_rows[at]] * (rows // 128), axis=1)
        sine = jnp.concatenate([sin_rows[at]] * (rows // 128), axis=1)
        mix = jnp.concatenate([pick_tok, low_rows[at]], axis=0)
        for h in range(heads):
            lanes = slice(h * HEAD_DIM, (h + 1) * HEAD_DIM)
            g = 0 if (h + 1) * HEAD_DIM <= cut else 1
            here = slice(h * HEAD_DIM - g * cut, (h + 1) * HEAD_DIM - g * cut)
            left_q = jnp.concatenate([rings[g][at, :, here], pack_q[:, lanes]], axis=0)
            q = dot(left_q, mix, ((0,), (0,)))
            low, high = q[:half], q[half:]
            q = jnp.concatenate(
                [low * cosine - high * sine, high * cosine + low * sine], axis=0
            ).astype(bf16)
            s = dot(keys[at], jnp.concatenate([q, pick_tok, filler], axis=0))
            e = jnp.exp2((s - jnp.max(s, axis=0, keepdims=True)) * scale).astype(bf16)
            out = dot(values[...], e)
            inverse = 1.0 / out[HEAD_DIM:HEAD_DIM + 1]
            mixed[lanes] = (out[:HEAD_DIM] * inverse).astype(bf16)

    def near_copy(at):
        return pltpu.make_async_remote_copy(
            src_ref=terms.at[at, 1 - lax.rem(mc, 2)], dst_ref=near_in.at[at],
            send_sem=near_send.at[at], recv_sem=near_recv.at[at],
            device_id={"mp": mc + 1 - 2 * lax.rem(mc, 2)}, device_id_type=MESH,
        )

    def far_copy(at):
        return pltpu.make_async_remote_copy(
            src_ref=far_out.at[at], dst_ref=far_in.at[at],
            send_sem=far_send.at[at], recv_sem=far_recv.at[at],
            device_id={"mp": lax.rem(mc + 2, n_mp)}, device_id_type=MESH,
        )

    def project(at):
        y = dot(wo_ref[...], mixed[...])
        low = jnp.where(same, y[cols:], 0.0)
        place = pl.ds(pl.multiple_of(at * own_tok, own_tok), own_tok)
        more = jnp.concatenate([right_o, right_o, right_o, goal[place, :]], axis=0)
        y = y[:cols] + dot(more, jnp.concatenate([*split3(low), pick_tok], axis=0), ((0,), (0,)))
        terms[at] = y.reshape(terms.shape[1:]).astype(bf16)
        near_copy(at).start()

    def join(at):
        near_copy(at).wait_recv()
        core, side = lax.rem(mc, 2), mc // 2
        own_sum[at] = terms[at, core, side].astype(f32) + near_in[at, side].astype(f32)
        far_out[at] = (
            terms[at, core, 1 - side].astype(f32) + near_in[at, 1 - side].astype(f32)
        ).astype(bf16)
        far_copy(at).start()

    def squares(at):
        far_copy(at).wait_recv()
        out = own_sum[at] + far_in[at].astype(f32)
        out = out * out
        more = total[...]
        for i in range(quarter // 8):
            more = more + out[i * 8:(i + 1) * 8]
        total[...] = more

    def block_of(j):
        away = (j + 1) // 2
        return pop_at(my_r + jnp.where(lax.rem(j, 2) == 1, -away, away))

    def arrive(j):
        direction, step = (j - 1) % 2, (j - 1) // 2
        if step == depth - 1:
            for d in range(2):
                hop(d, step, d).wait_recv()
            return
        for g in range(2):
            hop(direction, step, g).wait_recv()
            if hops(direction, step + 1, g):
                hop(direction, step + 1, g).start()

    def block(j, carry):
        for k in range(1, n_pop):
            pl.when(j == k)(functools.partial(arrive, k))
        at = block_of(j)
        attend(at)
        project(at)

        @pl.when(j >= 1)
        def _():
            join(block_of(j - 1))

        @pl.when(j >= 3)
        def _():
            squares(block_of(j - 3))

        return carry

    lax.fori_loop(0, n_pop, block, 0)
    join(block_of(n_pop - 1))
    for j in range(n_pop - 3, n_pop):
        squares(block_of(jnp.int32(j)))

    lane_row = lax.broadcasted_iota(jnp.int32, (1, 128), 1)
    sums = jnp.sum(total[...], axis=0, keepdims=True)
    member_of = lax.broadcasted_iota(jnp.int32, (1, rows), 1) // own_tok
    mine = jnp.zeros((1, 128), f32)
    for k in range(n_pop):
        value_k = jnp.sum(jnp.where(member_of == k, sums, 0.0), axis=1, keepdims=True)
        mine = mine + jnp.where(lane_row == k, value_k, 0.0)

    my_id = mc * n_pop + me
    errs[my_id] = mine

    def err_copy(i):
        other = lax.rem(my_id + i, n_dev)
        return pltpu.make_async_remote_copy(
            src_ref=errs.at[my_id], dst_ref=errs.at[my_id],
            send_sem=err_send.at[i], recv_sem=err_recv.at[i],
            device_id={"pop": lax.rem(other, n_pop), "mp": other // n_pop}, device_id_type=MESH,
        )

    def err_start(i, carry):
        err_copy(i).start()
        return carry

    def err_wait(i, carry):
        err_copy(i).wait_recv()
        return carry

    lax.fori_loop(1, n_dev, err_start, 0)
    for kind in range(6):
        for i in range(1, n_pop):
            to_pop(i, kind).wait_send()
    for step in range(depth):
        for g in range(2):
            for direction in range(2):
                if hops(direction, step, g):
                    hop(direction, step, g).wait_send()
    for at in range(n_pop):
        near_copy(at).wait_send()
        far_copy(at).wait_send()

    lax.fori_loop(1, n_dev, err_wait, 0)
    error = errs[0]
    for i in range(1, n_dev):
        error = error + errs[i]
    live = lane_row < n_pop
    fitness = -(error / (tok * width))
    mean = jnp.sum(jnp.where(live, fitness, 0.0), axis=1, keepdims=True) / n_pop
    dev = jnp.where(live, fitness - mean, 0.0)
    spread = jnp.sum(dev * dev, axis=1, keepdims=True) / n_pop
    weight = dev / jnp.sqrt(spread + spread_floor)
    stat_out[...] = jnp.concatenate(
        [fitness, weight, jnp.zeros((6, 128), f32)], axis=0
    )

    def err_drain(i, carry):
        err_copy(i).wait_send()
        return carry

    lax.fori_loop(1, n_dev, err_drain, 0)


def grad_kernel(a_ref, b_ref, stat_ref, gq_hbm, got_hbm, fit_ref, gq_ref, got_ref, sem):
    pack_a = a_ref[...]
    pack_b = b_ref[...].astype(f32)
    rows, cols = pack_b.shape
    row = lax.broadcasted_iota(jnp.int32, (rows, 128), 0)
    lane = lax.broadcasted_iota(jnp.int32, (rows, 128), 1)
    per_row = jnp.sum(jnp.where(lane == row // PACK, stat_ref[1:2, :], 0.0), axis=1, keepdims=True)
    per_row = per_row / (noise_scale * noise_scale)
    kind = lax.rem(lax.broadcasted_iota(jnp.int32, (rows, 1), 0), PACK)
    edges = (0, (cols // 2 + 127) // 128 * 128, cols)
    copies = []
    for out, target, weight in (
        (gq_ref, gq_hbm, jnp.where(kind < RANK, per_row, 0.0)),
        (got_ref, got_hbm, jnp.where(kind >= RANK, per_row, 0.0)),
    ):
        pieces = jnp.concatenate(split3(pack_b * weight), axis=0)
        right = jnp.concatenate([pack_a] * 3, axis=0)
        for low, high in zip(edges[:-1], edges[1:]):
            out[low:high, :] = dot(pieces[:, low:high], right, ((0,), (0,)))
            copy = pltpu.make_async_copy(
                out.at[low:high], target.at[low:high], sem.at[len(copies)]
            )
            copy.start()
            copies.append(copy)
    me = lax.axis_index("pop")
    fit_ref[0] = jnp.sum(jnp.where(lane[:1] == me, stat_ref[0:1, :], 0.0))
    for copy in copies:
        copy.wait()


def per_device_fast(
    n_pop, n_mp,
    tokens, target, w_query, w_key, w_value, w_out,
    query_left_factors, query_right_factors, o_left, o_right, member_ids,
):
    tok, width = tokens.shape
    feats = w_query.shape[1]
    cols = w_out.shape[1]
    own_tok = tok // n_pop
    rows = n_pop * own_tok
    cosine, sine = rope_tables(tok, HEAD_DIM)
    half = HEAD_DIM // 2
    by_row = lambda x: np.tile(
        x[:, half:].T.reshape(half, n_pop, own_tok).transpose(1, 0, 2), (1, 1, 128 // own_tok)
    )
    vmem = pl.BlockSpec(memory_space=pltpu.VMEM)
    hbm = pl.BlockSpec(memory_space=pltpu.HBM)
    smem = pl.BlockSpec(memory_space=pltpu.SMEM)
    dma = pltpu.SemaphoreType.DMA
    depth = n_pop // 2
    n_dev = n_pop * n_mp
    cut = (feats // HEAD_DIM + 1) // 2 * HEAD_DIM
    like = lambda x: pltpu.VMEM(x.shape, x.dtype)
    wot = w_out.T
    pack_a, pack_b, stat = pl.pallas_call(
        functools.partial(forward_kernel, n_pop, n_mp, width),
        name="forward",
        out_shape=(
            jax.ShapeDtypeStruct((n_pop * PACK, feats), bf16),
            jax.ShapeDtypeStruct((n_pop * PACK, cols), bf16),
            jax.ShapeDtypeStruct((8, 128), f32),
        ),
        in_specs=[hbm] * 6 + [vmem] * 4 + [smem] + [vmem] * 4,
        out_specs=(vmem, vmem, vmem),
        scratch_shapes=[
            like(tokens), like(w_query), pltpu.VMEM((width, 2 * HEAD_DIM), bf16),
            pltpu.VMEM((cols + n_pop * RANK, feats), bf16), like(target),
            pltpu.VMEM((n_pop, own_tok, cut), LINK),
            pltpu.VMEM((n_pop, own_tok, feats - cut), LINK),
            pltpu.VMEM((n_pop, own_tok, cut), LINK),
            pltpu.VMEM((n_pop, own_tok, feats - cut), LINK),
            pltpu.VMEM((RANK, tok), bf16),
            pltpu.VMEM((n_pop, RANK, tok), bf16),
            pltpu.VMEM((RANK, feats), bf16),
            pltpu.VMEM((n_pop, RANK, feats), bf16),
            pltpu.VMEM((RANK, feats), bf16),
            pltpu.VMEM((n_pop, RANK, feats), bf16),
            pltpu.VMEM((n_pop, PACK, cols), bf16),
            pltpu.VMEM((n_pop, PACK, cols), bf16),
            pltpu.VMEM((n_pop, own_tok, cut), LINK),
            pltpu.VMEM((n_pop, own_tok, feats - cut), LINK),
            pltpu.VMEM((n_pop, tok, 2 * HEAD_DIM), bf16),
            pltpu.VMEM((HEAD_DIM + 16, tok), bf16),
            pltpu.VMEM((n_pop, n_pop * RANK, rows), bf16),
            pltpu.VMEM((tok, cols), bf16),
            pltpu.VMEM((feats, rows), bf16),
            pltpu.VMEM((n_pop, 2, n_mp // 2, cols // n_mp, rows), bf16),
            pltpu.VMEM((n_pop, n_mp // 2, cols // n_mp, rows), bf16),
            pltpu.VMEM((n_pop, cols // n_mp, rows), bf16),
            pltpu.VMEM((n_pop, cols // n_mp, rows), bf16),
            pltpu.VMEM((n_pop, cols // n_mp, rows), f32),
            pltpu.VMEM((8, rows), f32),
            pltpu.VMEM((n_dev, 1, 128), f32),
            dma((6,)),
            dma((6, n_pop)), dma((6, n_pop)),
            dma((2, depth, 2)), dma((2, depth, 2)),
            dma((n_pop,)), dma((n_pop,)),
            dma((n_pop,)), dma((n_pop,)),
            dma((n_dev,)), dma((n_dev,)),
        ],
        compiler_params=pltpu.CompilerParams(
            collective_id=0, has_side_effects=True, vmem_limit_bytes=60 * 1024 * 1024
        ),
    )(tokens, w_query, w_key, w_value, wot, target,
      query_left_factors[0].T, query_right_factors[0], o_left[0].T, o_right[0], member_ids,
      jnp.asarray(cosine), jnp.asarray(sine), jnp.asarray(by_row(cosine)), jnp.asarray(by_row(sine)))
    grad = jax.ShapeDtypeStruct((cols, feats), f32)
    grad_query, grad_out_t, fitness = pl.pallas_call(
        grad_kernel,
        name="grads",
        out_shape=(grad, grad, jax.ShapeDtypeStruct((1,), f32)),
        in_specs=[vmem, vmem, vmem],
        out_specs=(hbm, hbm, smem),
        scratch_shapes=[like(grad), like(grad), dma((4,))],
    )(pack_a, pack_b, stat)
    return grad_query, grad_out_t.T, fitness


def tables(count, head_size):
    position = jnp.arange(count, dtype=jnp.float32)
    index = jnp.arange(head_size // 2, dtype=jnp.float32)
    freq = jnp.exp(-math.log(rope_base) * 2.0 * index / head_size)
    angle = position[:, None] * freq[None, :]
    return (jnp.cos(angle)[:, None, :], jnp.sin(angle)[:, None, :])


def rotate(field, cosine_table, sine):
    half = field.shape[-1] // 2
    first = field[..., :half]
    second = field[..., half:]
    return jnp.concatenate(
        [first * cosine_table - second * sine, second * cosine_table + first * sine], axis=-1
    )


def per_device(
    tokens,
    target,
    w_query,
    w_key,
    w_value,
    w_out,
    query_left_factors,
    query_right_factors,
    o_left,
    o_right,
    member_ids,
):
    tok = tokens.shape[0]
    local_feats = w_query.shape[1]
    local_kv = w_key.shape[1] // HEAD_DIM
    group = group_of(w_query, w_key)
    local_heads = local_kv * group
    slots = query_left_factors.shape[0]
    scale = HEAD_DIM ** (-0.5)
    cosine_table, sine = tables(tok, HEAD_DIM)
    base = jnp.dot(
        tokens,
        lax.all_gather(w_query, "pop", axis=0, tiled=True),
        preferred_element_type=jnp.float32,
    )
    keys = rotate(
        jnp.dot(tokens, w_key, preferred_element_type=jnp.float32).reshape(tok, local_kv, HEAD_DIM),
        cosine_table,
        sine,
    ).astype(jnp.bfloat16)
    values = (
        jnp.dot(tokens, w_value, preferred_element_type=jnp.float32)
        .astype(jnp.bfloat16)
        .reshape(tok, local_kv, HEAD_DIM)
    )
    signs = (1 - 2 * (member_ids % 2)).astype(jnp.float32)
    factor = noise_scale * signs[:, None, None]
    lowrank_product = jnp.einsum(
        "td,mdr->mtr", tokens, query_left_factors, preferred_element_type=jnp.float32
    ).astype(jnp.bfloat16)
    query = base[None] + factor * jnp.einsum(
        "olj,ojv->olv", lowrank_product, query_right_factors, preferred_element_type=jnp.float32
    )
    query = rotate(
        query.reshape(slots, tok, local_heads, HEAD_DIM), cosine_table[None], sine[None]
    ).astype(jnp.bfloat16)
    query = query.reshape(slots, tok, local_kv, group, HEAD_DIM)
    scores = jnp.einsum("mtkgd,skd->mkgts", query, keys, preferred_element_type=jnp.float32) * scale
    causal = jnp.arange(tok)[:, None] >= jnp.arange(tok)[None, :]
    scores = jnp.where(causal, scores, -1e30)
    probs = jax.nn.softmax(scores, axis=-1).astype(jnp.bfloat16)
    mixed = (
        jnp.einsum("mkgts,skd->mtkgd", probs, values, preferred_element_type=jnp.float32)
        .astype(jnp.bfloat16)
        .reshape(slots, tok, local_feats)
    )
    low_out = jnp.einsum("mtf,mfr->mtr", mixed, o_left, preferred_element_type=jnp.float32)
    right_full = o_right.astype(jnp.float32)
    part = jnp.einsum(
        "mtf,fe->mte",
        mixed,
        lax.all_gather(w_out, "pop", axis=1, tiled=True),
        preferred_element_type=jnp.float32,
    )
    term = part + factor * jnp.einsum(
        "mtr,mre->mte", low_out, right_full, precision=lax.Precision.HIGHEST
    )
    output = lax.psum_scatter(
        term.astype(jnp.bfloat16), "mp", scatter_dimension=2, tiled=True
    ).astype(jnp.float32)
    diff = output - target.astype(jnp.float32)[None]
    errors = lax.psum(jnp.sum(diff * diff, axis=(1, 2)), "mp")
    fitness = -(errors / (tok * tokens.shape[1]))
    count = slots * lax.axis_size("pop")
    mean = lax.psum(jnp.sum(fitness), "pop") / count
    spread = lax.psum(jnp.sum((fitness - mean) * (fitness - mean)), "pop") / count
    weight = signs * (fitness - mean) / jnp.sqrt(spread + spread_floor)
    every_weight = lax.all_gather(weight, "pop", axis=0, tiled=True)
    right_factors_gathered, left_all = (
        lax.all_gather(query_right_factors, "pop", axis=0, tiled=True),
        lax.all_gather(o_left, "pop", axis=0, tiled=True),
    )
    rows_q = lax.all_to_all(query_left_factors, "pop", split_axis=1, concat_axis=0, tiled=True)
    cols_o = lax.all_to_all(o_right, "pop", split_axis=2, concat_axis=0, tiled=True)
    whole_population = rows_q.shape[0]
    left_q = jnp.transpose(
        rows_q.astype(jnp.float32) * every_weight[:, None, None], (1, 0, 2)
    ).reshape(rows_q.shape[1], whole_population * RANK)
    right_q = right_factors_gathered.astype(jnp.float32).reshape(
        whole_population * RANK, local_feats
    )
    grad_query = jnp.dot(left_q, right_q, precision=lax.Precision.HIGHEST) / noise_scale
    output_left_factor = jnp.transpose(
        left_all.astype(jnp.float32) * every_weight[:, None, None], (1, 0, 2)
    ).reshape(local_feats, whole_population * RANK)
    right_o = cols_o.astype(jnp.float32).reshape(whole_population * RANK, cols_o.shape[2])
    grad_out = jnp.dot(output_left_factor, right_o, precision=lax.Precision.HIGHEST) / noise_scale
    return (grad_query, grad_out, fitness)


def group_of(w_query, w_key):
    return w_query.shape[1] // w_key.shape[1]


def pick(args, n_pop, n_mp):
    tok = args[0].shape[0]
    kernel = (
        args[6].shape[0] == n_pop
        and n_mp == 4
        and n_pop % n_mp == 0
        and n_pop % 2 == 0
        and n_pop * PACK <= 128
        and tok % (n_pop * 16) == 0
        and tok // n_pop < 128
        and 128 % (tok // n_pop) == 0
        and args[5].shape[1] // n_pop % (16 * n_mp) == 0
        and args[2].shape[1] // n_mp == 2 * args[5].shape[1] // n_pop
        and args[2].shape[0] == args[5].shape[1]
        and args[3].shape[1] == n_mp * HEAD_DIM
    )
    return functools.partial(per_device_fast, n_pop, n_mp) if kernel else per_device


def solution(mesh):
    placed = (
        P(),
        P(None, "mp"),
        P("pop", "mp"),
        P(None, "mp"),
        P(None, "mp"),
        P("mp", "pop"),
        P("pop", None, None),
        P("pop", None, "mp"),
        P("pop", "mp", None),
        P("pop", None, None),
        P("pop"),
    )
    n_pop, n_mp = mesh.shape["pop"], mesh.shape["mp"]

    def whole(*args):
        return jax.shard_map(
            pick(args, n_pop, n_mp),
            mesh=mesh,
            in_specs=placed,
            out_specs=(P("pop", "mp"), P("mp", "pop"), P("pop")),
            check_vma=False,
        )(*args)

    return whole
```

```python
import functools
import math

import jax
import jax.numpy as jnp
import numpy as np
from jax import lax
from jax.experimental import pallas as pl
from jax.experimental.pallas import tpu as pltpu
from jax.sharding import PartitionSpec as P

HEAD_DIM = 128
RANK = 4
PACK = 8
LINK = jnp.bfloat16

noise_scale = 0.5
rope_base = 1000000.0
spread_floor = 0.001
MESH = pl.DeviceIdType.MESH
f32 = jnp.float32
bf16 = jnp.bfloat16


def rope_tables(count, head_size):
    index = np.arange(head_size // 2, dtype=np.float64)
    freq = np.exp(-math.log(rope_base) * 2.0 * index / head_size)
    angle = np.arange(count, dtype=np.float64)[:, None] * freq[None, :]
    cosine, sine = np.cos(angle), np.sin(angle)
    return (
        np.concatenate([cosine, cosine], 1).astype(np.float32),
        np.concatenate([-sine, sine], 1).astype(np.float32),
    )


def dot(a, b, dims=((1,), (0,))):
    return lax.dot_general(a, b, (dims, ((), ())), preferred_element_type=f32)


def split3(x):
    hi = x.astype(bf16)
    rest = x - hi.astype(f32)
    mid = rest.astype(bf16)
    low = (rest - mid.astype(f32)).astype(bf16)
    return hi, mid, low


def forward_kernel(
    n_pop, n_mp, width,
    tok_hbm, wq_hbm, wk_hbm, wv_hbm, wo_hbm, tgt_hbm, ql_hbm, qr_hbm, ol_hbm, or_hbm,
    cos_hbm, sin_hbm, cos_rows_hbm, sin_rows_hbm, id_ref,
    pack_a_out, pack_b_out, stat_out,
    window, wq_ref, qr_ref, tok_ref, ql_ref, ol_ref, or_ref, kv_ref, cos_ref, sin_ref,
    tgt_ref, cos_rows, sin_rows, wo_ref,
    part, across_in, along_out, along_in, known, mine_l, packs_l, mine_q, packs_q,
    mine_o, packs_o, mine_b, packs_b,
    keys, values, low_rows, goal, queries, scores, peaks, exps, mixed, terms, near_in, far_out, far_in, own_sum, total, errs,
    load_sem, across_send, across_recv, along_send, along_recv,
    pop_send, pop_recv, known_send, known_recv, near_send, near_recv, far_send, far_recv, err_send, err_recv,
):
    me = lax.axis_index("pop")
    mc = lax.axis_index("mp")
    n_dev = n_pop * n_mp
    tok, feats = tok_ref.shape[0], wq_ref.shape[1]
    own_tok = tok // n_pop
    rows = n_pop * own_tok
    heads = feats // HEAD_DIM
    cols = wq_ref.shape[0]
    ranks = n_pop * RANK
    quarter = cols // n_mp
    odd = lax.rem(me, 2) == 1
    near_cols = pl.ds(pl.multiple_of(me // 2 * 2 * cols, 128), 2 * cols)
    loads = [
        pltpu.make_async_copy(src, dst, load_sem.at[i])
        for i, (src, dst) in enumerate((
            (tok_hbm.at[:, near_cols], window), (wq_hbm, wq_ref), (qr_hbm, qr_ref),
            (tok_hbm, tok_ref), (ql_hbm, ql_ref), (ol_hbm, ol_ref), (or_hbm, or_ref),
            (wk_hbm, kv_ref.at[:, :HEAD_DIM]), (wv_hbm, kv_ref.at[:, HEAD_DIM:]),
            (cos_hbm, cos_ref), (sin_hbm, sin_ref), (tgt_hbm, tgt_ref),
            (cos_rows_hbm, cos_rows), (sin_rows_hbm, sin_rows), (wo_hbm, wo_ref.at[:cols]),
        ))
    ]
    for load in loads[:3]:
        load.start()

    barrier = pltpu.get_barrier_semaphore()

    pops = [lax.rem(me + i, n_pop) for i in range(n_pop)]
    mps = [lax.rem(mc + i, n_mp) for i in range(n_mp)]
    others = [(p, m) for m in mps for p in pops][1:]
    for p, m in others:
        pl.semaphore_signal(
            barrier, inc=1, device_id={"pop": p, "mp": m}, device_id_type=MESH
        )

    sign = 1 - 2 * lax.rem(id_ref[0], 2)
    factor = noise_scale * sign.astype(f32)
    for load in loads[3:]:
        load.start()
    for load in loads[:3]:
        load.wait()
    wq = wq_ref[...]
    first, second = window[:, :cols], window[:, cols:]
    base = dot(jnp.where(odd, second, first), wq)
    for b in range(n_pop):
        part[b % 2, b // 2] = base[b * own_tok:(b + 1) * own_tok].astype(LINK)
    mine_q[...] = (qr_ref[...].astype(f32) * factor).astype(bf16)

    pl.semaphore_wait(barrier, n_dev - 1)

    side, level = lax.rem(me, 2), me // 2
    levels = n_pop // 2
    beside = me + 1 - 2 * side
    ways = [
        sorted(range(levels), key=lambda t: (-abs(t - u), (t < levels // 2) == (u < levels // 2)))
        for u in range(levels)
    ]

    def far(k):
        at = jnp.int32(ways[0][k])
        for u in range(1, levels):
            at = jnp.where(level == u, ways[u][k], at)
        return at

    fars = [far(k) for k in range(levels)]
    nears = fars[:-1][::-1]

    def across(k):
        return pltpu.make_async_remote_copy(
            src_ref=part.at[1 - side, fars[k]], dst_ref=across_in.at[fars[k]],
            send_sem=across_send, recv_sem=across_recv.at[k],
            device_id={"pop": beside}, device_id_type=MESH,
        )

    def along(k):
        return pltpu.make_async_remote_copy(
            src_ref=along_out.at[fars[k]], dst_ref=along_in.at[level],
            send_sem=along_send, recv_sem=along_recv,
            device_id={"pop": 2 * fars[k] + side}, device_id_type=MESH,
        )

    def relay(k):
        across(k).wait_recv()
        joined = part[side, fars[k]].astype(f32) + across_in[fars[k]].astype(f32)
        if k == levels - 1:
            return joined
        along_out[fars[k]] = joined.astype(LINK)
        along(k).start()

    gathered = ((mine_q, packs_q), (mine_l, packs_l), (mine_o, packs_o), (mine_b, packs_b))

    def to_all(kind):
        mine, packs = gathered[kind]
        for other in pops[1:]:
            pltpu.make_async_remote_copy(
                src_ref=mine.at[other] if kind == 3 else mine, dst_ref=packs.at[me],
                send_sem=pop_send.at[kind], recv_sem=pop_recv.at[kind],
                device_id={"pop": other}, device_id_type=MESH,
            ).start()

    def all_of(refs, send_sem, recv_sem):
        return pltpu.make_async_remote_copy(
            src_ref=refs, dst_ref=refs, send_sem=send_sem, recv_sem=recv_sem,
            device_id={"pop": beside}, device_id_type=MESH,
        )

    def packs_done(kind):
        return all_of(gathered[kind][1].at[:n_pop - 1], pop_send.at[kind], pop_recv.at[kind])

    across(0).start()
    to_all(0)
    for k in range(1, levels):
        across(k).start()
    for load in loads[3:7]:
        load.wait()
    ql = ql_ref[...]
    mine_l[...] = dot(ql, tok_ref[...], ((1,), (1,))).astype(bf16)
    to_all(1)
    mine_o[...] = ol_ref[...]
    both = jnp.concatenate([ql.astype(f32), or_ref[...].astype(f32) * factor], axis=0)
    for q in range(n_pop):
        mine_b[q] = both[:, q * cols:(q + 1) * cols].astype(bf16)
    packs_b[me] = mine_b[me]
    packs_l[me] = mine_l[...]
    packs_q[me] = mine_q[...]
    packs_o[me] = mine_o[...]

    for load in loads[7:11]:
        load.wait()
    pair = dot(tok_ref[...], kv_ref[...])
    key = pair[:, :HEAD_DIM]
    key = (key * cos_ref[...] + pltpu.roll(key, HEAD_DIM // 2, 1) * sin_ref[...]).astype(bf16)
    values[:HEAD_DIM] = pair[:, HEAD_DIM:].T.astype(bf16)
    values[HEAD_DIM:] = jnp.ones((values.shape[0] - HEAD_DIM, tok), bf16)
    relay(0)
    spot = lax.broadcasted_iota(jnp.int32, (tok, HEAD_DIM), 0)
    lane = lax.broadcasted_iota(jnp.int32, (tok, HEAD_DIM), 1)
    for q in range(n_pop):
        keys[q, :, :HEAD_DIM] = key
        hidden = (spot > q * own_tok + lane) & (lane < own_tok)
        keys[q, :, HEAD_DIM:] = jnp.where(hidden, -1e30, 0.0).astype(bf16)
    relay(1)

    loads[11].wait()
    owner = me // (n_pop // n_mp)
    tgt = jnp.where(odd, tgt_ref[:, cols:], tgt_ref[:, :cols])
    goal[...] = jnp.where(mc == owner, -tgt, jnp.zeros_like(tgt))

    row_tok = lax.rem(lax.broadcasted_iota(jnp.int32, (own_tok, rows), 1), own_tok)
    pick_tok = (row_tok == lax.broadcasted_iota(jnp.int32, (own_tok, rows), 0)).astype(bf16)
    row_member = lax.broadcasted_iota(jnp.int32, (ranks, rows), 1) // own_tok
    same = row_member == lax.broadcasted_iota(jnp.int32, (ranks, rows), 0) // RANK

    def stacked(parts, *more):
        return jnp.concatenate(
            [p[i].astype(f32) for i in range(n_pop) for p in (parts,) + more], axis=0
        ).astype(bf16)

    filler = jnp.zeros((keys.shape[2] - HEAD_DIM - own_tok, rows), bf16)
    for slot in range(2):
        for h in range(heads):
            queries[slot, h, HEAD_DIM:HEAD_DIM + own_tok] = pick_tok
            queries[slot, h, HEAD_DIM + own_tok:] = filler
    total[...] = jnp.zeros_like(total)
    for k in range(2, levels - 1):
        relay(k)
    own_base = relay(levels - 1)
    to_all(2)
    to_all(3)
    packs_done(0).wait_recv()
    packs_done(1).wait_recv()
    pack_q = stacked(packs_q)
    low_all = stacked(packs_l)
    spot = lax.broadcasted_iota(jnp.int32, (tok, rows), 0)
    at_tok = lax.rem(lax.broadcasted_iota(jnp.int32, (tok, rows), 1), own_tok)
    for q in range(n_pop):
        sel = (spot == at_tok + q * own_tok).astype(bf16)
        low_rows[q] = jnp.where(same, dot(low_all, sel), 0.0).astype(bf16)

    def share(at, other):
        return pltpu.make_async_remote_copy(
            src_ref=known.at[at], dst_ref=known.at[at],
            send_sem=known_send, recv_sem=known_recv.at[at],
            device_id={"pop": other}, device_id_type=MESH,
        )

    loads[12].wait()
    loads[13].wait()
    all_of(along_in.at[:levels - 1], along_send, along_recv).wait_recv()
    for k in range(levels - 1):
        own_base = own_base + along_in[fars[k]].astype(f32)
    known[me] = own_base.astype(LINK)
    share(me, beside).start()
    for near in nears:
        share(me, 2 * near + side).start()

    scale = HEAD_DIM ** (-0.5) * math.log2(math.e)
    half = HEAD_DIM // 2
    def attend(*group):
        for slot, at in enumerate(group):
            cosine = jnp.concatenate([cos_rows[at]] * (rows // 128), axis=1)
            sine = jnp.concatenate([sin_rows[at]] * (rows // 128), axis=1)
            mix = jnp.concatenate([pick_tok, low_rows[at]], axis=0)
            q_all = dot(jnp.concatenate([known[at], pack_q], axis=0), mix, ((0,), (0,)))
            for h in range(heads):
                low = q_all[h * HEAD_DIM:h * HEAD_DIM + half]
                high = q_all[h * HEAD_DIM + half:(h + 1) * HEAD_DIM]
                queries[slot, h, :half] = (low * cosine - high * sine).astype(bf16)
                queries[slot, h, half:HEAD_DIM] = (high * cosine + low * sine).astype(bf16)
        for slot, at in enumerate(group):
            for h in range(heads):
                s = dot(keys[at], queries[slot, h])
                scores[slot, h] = s
                peak = s[:8]
                for i in range(8, tok, 8):
                    peak = jnp.maximum(peak, s[i:i + 8])
                peaks[slot, h] = peak
        for slot, at in enumerate(group):
            for h in range(heads):
                peak = jnp.max(peaks[slot, h], axis=0, keepdims=True)
                exps[slot, h] = jnp.exp2((scores[slot, h] - peak) * scale).astype(bf16)
        for slot, at in enumerate(group):
            for h in range(heads):
                out = dot(values[...], exps[slot, h])
                inverse = 1.0 / out[HEAD_DIM:HEAD_DIM + 1]
                mixed[slot, h * HEAD_DIM:(h + 1) * HEAD_DIM] = (
                    out[:HEAD_DIM] * inverse
                ).astype(bf16)

    def near_copy(at):
        return pltpu.make_async_remote_copy(
            src_ref=terms.at[at, 1 - lax.rem(mc, 2)], dst_ref=near_in.at[at],
            send_sem=near_send, recv_sem=near_recv.at[at],
            device_id={"mp": mc + 1 - 2 * lax.rem(mc, 2)}, device_id_type=MESH,
        )

    def far_copy(at):
        return pltpu.make_async_remote_copy(
            src_ref=far_out.at[at], dst_ref=far_in.at[at],
            send_sem=far_send, recv_sem=far_recv.at[at],
            device_id={"mp": lax.rem(mc + 2, n_mp)}, device_id_type=MESH,
        )

    def project(*group):
        lows = [
            jnp.where(same, dot(wo_ref[cols:], mixed[slot]), 0.0) for slot in range(len(group))
        ]
        for slot, at in enumerate(group):
            place = pl.ds(pl.multiple_of(at * own_tok, own_tok), own_tok)
            more = jnp.concatenate([right_o, right_o, right_o, goal[place, :]], axis=0)
            low = jnp.concatenate([*split3(lows[slot]), pick_tok], axis=0)
            y = dot(wo_ref[:cols], mixed[slot]) + dot(more, low, ((0,), (0,)))
            terms[at] = y.reshape(terms.shape[1:]).astype(bf16)
        for at in group:
            near_copy(at).start()

    def join(at):
        near_copy(at).wait_recv()
        core, side = lax.rem(mc, 2), mc // 2
        own_sum[at] = terms[at, core, side].astype(f32) + near_in[at, side].astype(f32)
        far_out[at] = (
            terms[at, core, 1 - side].astype(f32) + near_in[at, 1 - side].astype(f32)
        ).astype(bf16)
        far_copy(at).start()

    def squares(at):
        far_copy(at).wait_recv()
        out = own_sum[at] + far_in[at].astype(f32)
        out = out * out
        more = total[...]
        for i in range(quarter // 8):
            more = more + out[i * 8:(i + 1) * 8]
        total[...] = more

    attend(me)
    packs_done(2).wait_recv()
    packs_done(3).wait_recv()
    pack_a_out[...] = stacked(packs_q, packs_o)
    pack_b_out[...] = stacked(packs_b)
    right_o = jnp.concatenate(
        [packs_b[i, RANK:].astype(f32) for i in range(n_pop)], axis=0
    ).astype(bf16)
    loads[14].wait()
    wo_ref[cols:] = stacked(packs_o)
    project(me)

    def expect(at, pass_on):
        share(at, beside).wait_recv()
        if pass_on:
            share(at, beside).start()

    column = [2 * near + side for near in nears]
    beyond = [2 * near + 1 - side for near in nears]
    groups = [(me,), (beside, column[0])]
    for i in range(1, levels - 1):
        groups.append((column[i], beyond[i - 1]))
    groups.append((beyond[levels - 2],))
    expect(beside, False)
    expect(column[0], True)
    for k in range(1, len(groups)):
        if k >= 2:
            expect(beyond[k - 2], False)
        attend(*groups[k])
        if k < levels - 1:
            expect(column[k], True)
        for at in groups[k - 1]:
            join(at)
        project(*groups[k])
        if k >= 2:
            for at in groups[k - 2]:
                squares(at)
    for at in groups[-1]:
        join(at)
    for group in groups[-2:]:
        for at in group:
            squares(at)

    lane_row = lax.broadcasted_iota(jnp.int32, (1, 128), 1)
    sums = jnp.sum(total[...], axis=0, keepdims=True)
    member_of = lax.broadcasted_iota(jnp.int32, (1, rows), 1) // own_tok
    mine = jnp.zeros((1, 128), f32)
    for k in range(n_pop):
        value_k = jnp.sum(jnp.where(member_of == k, sums, 0.0), axis=1, keepdims=True)
        mine = mine + jnp.where(lane_row == k, value_k, 0.0)

    my_id = mc * n_pop + me
    errs[my_id] = mine

    for p, m in others:
        pltpu.make_async_remote_copy(
            src_ref=errs.at[my_id], dst_ref=errs.at[my_id], send_sem=err_send, recv_sem=err_recv,
            device_id={"pop": p, "mp": m}, device_id_type=MESH,
        ).start()
    all_errs = all_of(errs.at[:n_dev - 1], err_send, err_recv)
    for kind in range(len(gathered)):
        packs_done(kind).wait_send()
    all_of(part.at[0], across_send, across_recv.at[0]).wait_send()
    all_of(along_out.at[:levels - 1], along_send, along_recv).wait_send()
    all_of(known.at[:n_pop - 1], known_send, known_recv.at[0]).wait_send()
    all_of(near_in, near_send, near_recv.at[0]).wait_send()
    all_of(far_in, far_send, far_recv.at[0]).wait_send()
    all_errs.wait_recv()
    error = errs[0]
    for i in range(1, n_dev):
        error = error + errs[i]
    live = lane_row < n_pop
    fitness = -(error / (tok * width))
    mean = jnp.sum(jnp.where(live, fitness, 0.0), axis=1, keepdims=True) / n_pop
    dev = jnp.where(live, fitness - mean, 0.0)
    spread = jnp.sum(dev * dev, axis=1, keepdims=True) / n_pop
    weight = dev / jnp.sqrt(spread + spread_floor)
    stat_out[...] = jnp.concatenate(
        [fitness, weight, jnp.zeros((6, 128), f32)], axis=0
    )

    all_errs.wait_send()


def grad_kernel(a_ref, b_ref, stat_ref, gq_hbm, got_hbm, fit_ref, gq_ref, got_ref, sem):
    pack_a = a_ref[...]
    pack_b = b_ref[...].astype(f32)
    rows, cols = pack_b.shape
    row = lax.broadcasted_iota(jnp.int32, (rows, 128), 0)
    lane = lax.broadcasted_iota(jnp.int32, (rows, 128), 1)
    per_row = jnp.sum(jnp.where(lane == row // PACK, stat_ref[1:2, :], 0.0), axis=1, keepdims=True)
    per_row = per_row / (noise_scale * noise_scale)
    kind = lax.rem(lax.broadcasted_iota(jnp.int32, (rows, 1), 0), PACK)
    edges = (0, (cols // 2 + 127) // 128 * 128, cols)
    copies = []
    for out, target, weight in (
        (gq_ref, gq_hbm, jnp.where(kind < RANK, per_row, 0.0)),
        (got_ref, got_hbm, jnp.where(kind >= RANK, per_row, 0.0)),
    ):
        pieces = jnp.concatenate(split3(pack_b * weight), axis=0)
        right = jnp.concatenate([pack_a] * 3, axis=0)
        for low, high in zip(edges[:-1], edges[1:]):
            out[low:high, :] = dot(pieces[:, low:high], right, ((0,), (0,)))
            copy = pltpu.make_async_copy(
                out.at[low:high], target.at[low:high], sem.at[len(copies)]
            )
            copy.start()
            copies.append(copy)
    me = lax.axis_index("pop")
    fit_ref[0] = jnp.sum(jnp.where(lane[:1] == me, stat_ref[0:1, :], 0.0))
    for copy in copies:
        copy.wait()


def per_device_fast(
    n_pop, n_mp,
    tokens, target, w_query, w_key, w_value, w_out,
    query_left_factors, query_right_factors, o_left, o_right, member_ids,
):
    tok, width = tokens.shape
    feats = w_query.shape[1]
    cols = w_out.shape[1]
    own_tok = tok // n_pop
    rows = n_pop * own_tok
    cosine, sine = rope_tables(tok, HEAD_DIM)
    half = HEAD_DIM // 2
    by_row = lambda x: np.tile(
        x[:, half:].T.reshape(half, n_pop, own_tok).transpose(1, 0, 2), (1, 1, 128 // own_tok)
    )
    vmem = pl.BlockSpec(memory_space=pltpu.VMEM)
    hbm = pl.BlockSpec(memory_space=pltpu.HBM)
    smem = pl.BlockSpec(memory_space=pltpu.SMEM)
    dma = pltpu.SemaphoreType.DMA
    n_dev = n_pop * n_mp
    like = lambda x: pltpu.VMEM(x.shape, x.dtype)
    wot = w_out.T
    pack_a, pack_b, stat = pl.pallas_call(
        functools.partial(forward_kernel, n_pop, n_mp, width),
        name="forward",
        out_shape=(
            pltpu.VMEM((n_pop * PACK, feats), bf16),
            pltpu.VMEM((n_pop * PACK, cols), bf16),
            pltpu.VMEM((8, 128), f32),
        ),
        in_specs=[hbm] * 14 + [smem],
        out_specs=(vmem, vmem, vmem),
        scratch_shapes=[
            pltpu.VMEM((tok, 2 * cols), bf16), like(w_query), pltpu.VMEM((RANK, feats), bf16),
            like(tokens), pltpu.VMEM((RANK, width), bf16),
            pltpu.VMEM((RANK, feats), bf16), pltpu.VMEM((RANK, width), bf16),
            pltpu.VMEM((width, 2 * HEAD_DIM), bf16),
            pltpu.VMEM((tok, HEAD_DIM), f32), pltpu.VMEM((tok, HEAD_DIM), f32), like(target),
            pltpu.VMEM((n_pop, HEAD_DIM // 2, 128), f32),
            pltpu.VMEM((n_pop, HEAD_DIM // 2, 128), f32),
            pltpu.VMEM((cols + n_pop * RANK, feats), bf16),
            pltpu.VMEM((2, n_pop // 2, own_tok, feats), LINK),
            pltpu.VMEM((n_pop // 2, own_tok, feats), LINK),
            pltpu.VMEM((n_pop // 2, own_tok, feats), LINK),
            pltpu.VMEM((n_pop // 2, own_tok, feats), LINK),
            pltpu.VMEM((n_pop, own_tok, feats), LINK),
            pltpu.VMEM((RANK, tok), bf16),
            pltpu.VMEM((n_pop, RANK, tok), bf16),
            pltpu.VMEM((RANK, feats), bf16),
            pltpu.VMEM((n_pop, RANK, feats), bf16),
            pltpu.VMEM((RANK, feats), bf16),
            pltpu.VMEM((n_pop, RANK, feats), bf16),
            pltpu.VMEM((n_pop, PACK, cols), bf16),
            pltpu.VMEM((n_pop, PACK, cols), bf16),
            pltpu.VMEM((n_pop, tok, 2 * HEAD_DIM), bf16),
            pltpu.VMEM((HEAD_DIM + 16, tok), bf16),
            pltpu.VMEM((n_pop, n_pop * RANK, rows), bf16),
            pltpu.VMEM((tok, cols), bf16),
            pltpu.VMEM((2, feats // HEAD_DIM, 2 * HEAD_DIM, rows), bf16),
            pltpu.VMEM((2, feats // HEAD_DIM, tok, rows), f32),
            pltpu.VMEM((2, feats // HEAD_DIM, 8, rows), f32),
            pltpu.VMEM((2, feats // HEAD_DIM, tok, rows), bf16),
            pltpu.VMEM((2, feats, rows), bf16),
            pltpu.VMEM((n_pop, 2, n_mp // 2, cols // n_mp, rows), bf16),
            pltpu.VMEM((n_pop, n_mp // 2, cols // n_mp, rows), bf16),
            pltpu.VMEM((n_pop, cols // n_mp, rows), bf16),
            pltpu.VMEM((n_pop, cols // n_mp, rows), bf16),
            pltpu.VMEM((n_pop, cols // n_mp, rows), f32),
            pltpu.VMEM((8, rows), f32),
            pltpu.VMEM((n_dev, 1, 128), f32),
            dma((15,)),
            dma, dma((n_pop // 2,)), dma, dma,
            dma((4,)), dma((4,)), dma, dma((n_pop,)),
            dma, dma((n_pop,)), dma, dma((n_pop,)),
            dma, dma,
        ],
        compiler_params=pltpu.CompilerParams(
            collective_id=0, has_side_effects=True, vmem_limit_bytes=60 * 1024 * 1024
        ),
    )(tokens, w_query, w_key, w_value, wot, target,
      query_left_factors[0].T, query_right_factors[0], o_left[0].T, o_right[0],
      jnp.asarray(cosine), jnp.asarray(sine), jnp.asarray(by_row(cosine)), jnp.asarray(by_row(sine)),
      member_ids)
    grad = jax.ShapeDtypeStruct((cols, feats), f32)
    grad_query, grad_out_t, fitness = pl.pallas_call(
        grad_kernel,
        name="grads",
        out_shape=(grad, grad, jax.ShapeDtypeStruct((1,), f32)),
        in_specs=[vmem, vmem, vmem],
        out_specs=(hbm, hbm, smem),
        scratch_shapes=[like(grad), like(grad), dma((4,))],
        compiler_params=pltpu.CompilerParams(vmem_limit_bytes=16 * 1024 * 1024),
    )(pack_a, pack_b, stat)
    return grad_query, grad_out_t.T, fitness


def tables(count, head_size):
    position = jnp.arange(count, dtype=jnp.float32)
    index = jnp.arange(head_size // 2, dtype=jnp.float32)
    freq = jnp.exp(-math.log(rope_base) * 2.0 * index / head_size)
    angle = position[:, None] * freq[None, :]
    return (jnp.cos(angle)[:, None, :], jnp.sin(angle)[:, None, :])


def rotate(field, cosine_table, sine):
    half = field.shape[-1] // 2
    first = field[..., :half]
    second = field[..., half:]
    return jnp.concatenate(
        [first * cosine_table - second * sine, second * cosine_table + first * sine], axis=-1
    )


def per_device(
    tokens,
    target,
    w_query,
    w_key,
    w_value,
    w_out,
    query_left_factors,
    query_right_factors,
    o_left,
    o_right,
    member_ids,
):
    tok = tokens.shape[0]
    local_feats = w_query.shape[1]
    local_kv = w_key.shape[1] // HEAD_DIM
    group = group_of(w_query, w_key)
    local_heads = local_kv * group
    slots = query_left_factors.shape[0]
    scale = HEAD_DIM ** (-0.5)
    cosine_table, sine = tables(tok, HEAD_DIM)
    base = jnp.dot(
        tokens,
        lax.all_gather(w_query, "pop", axis=0, tiled=True),
        preferred_element_type=jnp.float32,
    )
    keys = rotate(
        jnp.dot(tokens, w_key, preferred_element_type=jnp.float32).reshape(tok, local_kv, HEAD_DIM),
        cosine_table,
        sine,
    ).astype(jnp.bfloat16)
    values = (
        jnp.dot(tokens, w_value, preferred_element_type=jnp.float32)
        .astype(jnp.bfloat16)
        .reshape(tok, local_kv, HEAD_DIM)
    )
    signs = (1 - 2 * (member_ids % 2)).astype(jnp.float32)
    factor = noise_scale * signs[:, None, None]
    lowrank_product = jnp.einsum(
        "td,mdr->mtr", tokens, query_left_factors, preferred_element_type=jnp.float32
    ).astype(jnp.bfloat16)
    query = base[None] + factor * jnp.einsum(
        "olj,ojv->olv", lowrank_product, query_right_factors, preferred_element_type=jnp.float32
    )
    query = rotate(
        query.reshape(slots, tok, local_heads, HEAD_DIM), cosine_table[None], sine[None]
    ).astype(jnp.bfloat16)
    query = query.reshape(slots, tok, local_kv, group, HEAD_DIM)
    scores = jnp.einsum("mtkgd,skd->mkgts", query, keys, preferred_element_type=jnp.float32) * scale
    causal = jnp.arange(tok)[:, None] >= jnp.arange(tok)[None, :]
    scores = jnp.where(causal, scores, -1e30)
    probs = jax.nn.softmax(scores, axis=-1).astype(jnp.bfloat16)
    mixed = (
        jnp.einsum("mkgts,skd->mtkgd", probs, values, preferred_element_type=jnp.float32)
        .astype(jnp.bfloat16)
        .reshape(slots, tok, local_feats)
    )
    low_out = jnp.einsum("mtf,mfr->mtr", mixed, o_left, preferred_element_type=jnp.float32)
    right_full = o_right.astype(jnp.float32)
    part = jnp.einsum(
        "mtf,fe->mte",
        mixed,
        lax.all_gather(w_out, "pop", axis=1, tiled=True),
        preferred_element_type=jnp.float32,
    )
    term = part + factor * jnp.einsum(
        "mtr,mre->mte", low_out, right_full, precision=lax.Precision.HIGHEST
    )
    output = lax.psum_scatter(
        term.astype(jnp.bfloat16), "mp", scatter_dimension=2, tiled=True
    ).astype(jnp.float32)
    diff = output - target.astype(jnp.float32)[None]
    errors = lax.psum(jnp.sum(diff * diff, axis=(1, 2)), "mp")
    fitness = -(errors / (tok * tokens.shape[1]))
    count = slots * lax.axis_size("pop")
    mean = lax.psum(jnp.sum(fitness), "pop") / count
    spread = lax.psum(jnp.sum((fitness - mean) * (fitness - mean)), "pop") / count
    weight = signs * (fitness - mean) / jnp.sqrt(spread + spread_floor)
    every_weight = lax.all_gather(weight, "pop", axis=0, tiled=True)
    right_factors_gathered, left_all = (
        lax.all_gather(query_right_factors, "pop", axis=0, tiled=True),
        lax.all_gather(o_left, "pop", axis=0, tiled=True),
    )
    rows_q = lax.all_to_all(query_left_factors, "pop", split_axis=1, concat_axis=0, tiled=True)
    cols_o = lax.all_to_all(o_right, "pop", split_axis=2, concat_axis=0, tiled=True)
    whole_population = rows_q.shape[0]
    left_q = jnp.transpose(
        rows_q.astype(jnp.float32) * every_weight[:, None, None], (1, 0, 2)
    ).reshape(rows_q.shape[1], whole_population * RANK)
    right_q = right_factors_gathered.astype(jnp.float32).reshape(
        whole_population * RANK, local_feats
    )
    grad_query = jnp.dot(left_q, right_q, precision=lax.Precision.HIGHEST) / noise_scale
    output_left_factor = jnp.transpose(
        left_all.astype(jnp.float32) * every_weight[:, None, None], (1, 0, 2)
    ).reshape(local_feats, whole_population * RANK)
    right_o = cols_o.astype(jnp.float32).reshape(whole_population * RANK, cols_o.shape[2])
    grad_out = jnp.dot(output_left_factor, right_o, precision=lax.Precision.HIGHEST) / noise_scale
    return (grad_query, grad_out, fitness)


def group_of(w_query, w_key):
    return w_query.shape[1] // w_key.shape[1]


def pick(args, n_pop, n_mp):
    tok = args[0].shape[0]
    kernel = (
        args[6].shape[0] == n_pop
        and n_mp == 4
        and n_pop % n_mp == 0
        and n_pop % 2 == 0
        and n_pop * PACK <= 128
        and tok % (n_pop * 16) == 0
        and tok // n_pop < 128
        and 128 % (tok // n_pop) == 0
        and args[5].shape[1] // n_pop % (16 * n_mp) == 0
        and args[2].shape[1] // n_mp == 2 * args[5].shape[1] // n_pop
        and args[2].shape[0] == args[5].shape[1]
        and args[3].shape[1] == n_mp * HEAD_DIM
    )
    return functools.partial(per_device_fast, n_pop, n_mp) if kernel else per_device


def solution(mesh):
    placed = (
        P(),
        P(None, "mp"),
        P("pop", "mp"),
        P(None, "mp"),
        P(None, "mp"),
        P("mp", "pop"),
        P("pop", None, None),
        P("pop", None, "mp"),
        P("pop", "mp", None),
        P("pop", None, None),
        P("pop"),
    )
    n_pop, n_mp = mesh.shape["pop"], mesh.shape["mp"]

    def whole(*args):
        return jax.shard_map(
            pick(args, n_pop, n_mp),
            mesh=mesh,
            in_specs=placed,
            out_specs=(P("pop", "mp"), P("mp", "pop"), P("pop")),
            check_vma=False,
        )(*args)

    return whole
```

```python
import functools
import math

import jax
import jax.numpy as jnp
import numpy as np
from jax import lax
from jax.experimental import pallas as pl
from jax.experimental.pallas import tpu as pltpu
from jax.sharding import PartitionSpec as P

HEAD_DIM = 128
RANK = 4
PACK = 8
LINK = jnp.bfloat16

noise_scale = 0.5
rope_base = 1000000.0
spread_floor = 0.001
MESH = pl.DeviceIdType.MESH
f32 = jnp.float32
bf16 = jnp.bfloat16


def rope_tables(count, head_size):
    index = np.arange(head_size // 2, dtype=np.float64)
    freq = np.exp(-math.log(rope_base) * 2.0 * index / head_size)
    angle = np.arange(count, dtype=np.float64)[:, None] * freq[None, :]
    cosine, sine = np.cos(angle), np.sin(angle)
    return (
        np.concatenate([cosine, cosine], 1).astype(np.float32),
        np.concatenate([-sine, sine], 1).astype(np.float32),
    )


def dot(a, b, dims=((1,), (0,))):
    return lax.dot_general(a, b, (dims, ((), ())), preferred_element_type=f32)


def split3(x):
    hi = x.astype(bf16)
    rest = x - hi.astype(f32)
    mid = rest.astype(bf16)
    low = (rest - mid.astype(f32)).astype(bf16)
    return hi, mid, low


def forward_kernel(
    n_pop, n_mp, width,
    tok_hbm, wq_hbm, wk_hbm, wv_hbm, wo_hbm, tgt_hbm, ql_hbm, qr_hbm, ol_hbm, or_hbm,
    cos_hbm, sin_hbm, cos_rows_hbm, sin_rows_hbm, id_hbm,
    rows_out, left_out, stat_out,
    id_ref, window, wq_ref, qr_ref, tok_ref, ql_ref, ol_ref, or_ref, kv_ref, cos_ref, sin_ref,
    tgt_ref, cos_rows, sin_rows, wo_ref,
    part, across_in, along_out, along_in, own_base, known, mine_l, packs_l, mine_q, packs_q,
    mine_o, packs_o, mine_b, packs_b, mine_a, packs_a,
    keys, values, low_rows, goal, queries, scores, peaks, exps, mixed, terms, near_in, far_out, far_in, own_sum, total, errs,
    load_sem, across_send, across_recv, along_send, along_recv,
    pop_send, pop_recv, known_send, known_recv, near_send, near_recv, far_send, far_recv, err_send, err_recv,
):
    me = lax.axis_index("pop")
    mc = lax.axis_index("mp")
    n_dev = n_pop * n_mp
    tok, feats = tok_ref.shape[0], wq_ref.shape[1]
    own_tok = tok // n_pop
    rows = n_pop * own_tok
    heads = feats // HEAD_DIM
    cols = wo_hbm.shape[0]
    ranks = n_pop * RANK
    quarter = cols // n_mp
    odd = lax.rem(me, 2) == 1
    lead = wq_ref.shape[0] - cols
    near_cols = pl.ds(pl.multiple_of(me * cols - jnp.where(odd, lead, 0), 128), cols + lead)
    near_rows = pl.ds(pl.multiple_of(jnp.where(odd, lead, 0), 16), cols)
    loads = [
        pltpu.make_async_copy(src, dst, load_sem.at[i])
        for i, (src, dst) in enumerate((
            (tok_hbm.at[:, near_cols], window), (wq_hbm, wq_ref.at[near_rows]), (qr_hbm, qr_ref),
            (tok_hbm, tok_ref), (ql_hbm, ql_ref), (ol_hbm, ol_ref), (or_hbm, or_ref),
            (wk_hbm, kv_ref.at[:, :HEAD_DIM]), (wv_hbm, kv_ref.at[:, HEAD_DIM:]),
            (cos_hbm, cos_ref), (sin_hbm, sin_ref), (tgt_hbm, tgt_ref),
            (cos_rows_hbm, cos_rows), (sin_rows_hbm, sin_rows), (wo_hbm, wo_ref.at[:cols]),
            (id_hbm, id_ref),
        ))
    ]
    for load in loads[:3] + loads[15:]:
        load.start()

    barrier = pltpu.get_barrier_semaphore()

    pops = [lax.rem(me + i, n_pop) for i in range(n_pop)]
    mps = [lax.rem(mc + i, n_mp) for i in range(n_mp)]
    others = [(p, m) for m in mps for p in pops][1:]
    side, level = lax.rem(me, 2), me // 2
    levels = n_pop // 2
    beside = me + 1 - 2 * side
    aligned = [2 * lax.rem(level + i, levels) + side for i in range(1, levels)]
    near_mp, far_mp = mc + 1 - 2 * lax.rem(mc, 2), lax.rem(mc + 2, n_mp)
    partners = [(p, mc) for p in aligned[::-1] + [beside]] + [(me, near_mp), (me, far_mp)]
    for p, m in partners:
        pl.semaphore_signal(
            barrier, inc=1, device_id={"pop": p, "mp": m}, device_id_type=MESH
        )

    if lead:
        wq_ref[pl.ds(pl.multiple_of(jnp.where(odd, 0, cols), 16), lead), :] = jnp.zeros(
            (lead, feats), bf16
        )
    for load in loads[3:15]:
        load.start()
    for load in loads[:3] + loads[15:]:
        load.wait()
    sign = 1 - 2 * lax.rem(id_ref[0], 2)
    factor = noise_scale * sign.astype(f32)
    base = dot(window[...], wq_ref[...])
    for b in range(n_pop):
        part[b % 2, b // 2] = base[b * own_tok:(b + 1) * own_tok].astype(LINK)
    mine_q[...] = (qr_ref[...].astype(f32) * factor).astype(bf16)

    pl.semaphore_wait(barrier, len(partners))

    ways = [
        sorted(range(levels), key=lambda t: (-abs(t - u), (t < levels // 2) == (u < levels // 2)))
        for u in range(levels)
    ]

    def far(k):
        at = jnp.int32(ways[0][k])
        for u in range(1, levels):
            at = jnp.where(level == u, ways[u][k], at)
        return at

    fars = [far(k) for k in range(levels)]
    nears = fars[:-1][::-1]

    cut = (heads + 1) // 2 * HEAD_DIM
    halves = (slice(0, cut), slice(cut, feats))

    def across(k, g):
        return pltpu.make_async_remote_copy(
            src_ref=part.at[1 - side, fars[k], :, halves[g]],
            dst_ref=across_in.at[fars[k], :, halves[g]],
            send_sem=across_send, recv_sem=across_recv.at[k, g],
            device_id={"pop": beside}, device_id_type=MESH,
        )

    def along(k, g):
        return pltpu.make_async_remote_copy(
            src_ref=along_out.at[fars[k], :, halves[g]],
            dst_ref=along_in.at[level, :, halves[g]],
            send_sem=along_send, recv_sem=along_recv,
            device_id={"pop": 2 * fars[k] + side}, device_id_type=MESH,
        )

    def relay(k):
        for g, lanes in enumerate(halves):
            across(k, g).wait_recv()
            joined = part[side, fars[k], :, lanes].astype(f32)
            joined = joined + across_in[fars[k], :, lanes].astype(f32)
            if k == levels - 1:
                own_base[:, lanes] = joined
            else:
                along_out[fars[k], :, lanes] = joined.astype(LINK)
                along(k, g).start()

    gathered = ((mine_q, packs_q), (mine_l, packs_l), (mine_o, packs_o), (mine_b, packs_b),
                (mine_a, packs_a))

    crossed = [2 * lax.rem(level + i, levels) + 1 - side for i in range(levels)]

    def give(kind, places):
        mine, packs = gathered[kind]
        for other in places:
            pltpu.make_async_remote_copy(
                src_ref=mine.at[other] if kind >= 3 else mine, dst_ref=packs.at[me],
                send_sem=pop_send.at[kind], recv_sem=pop_recv.at[kind],
                device_id={"pop": other}, device_id_type=MESH,
            ).start()

    def all_of(refs, send_sem, recv_sem):
        return pltpu.make_async_remote_copy(
            src_ref=refs, dst_ref=refs, send_sem=send_sem, recv_sem=recv_sem,
            device_id={"pop": beside}, device_id_type=MESH,
        )

    def packs_done(kind):
        return all_of(gathered[kind][1].at[:n_pop - 1], pop_send.at[kind], pop_recv.at[kind])

    for g in range(2):
        across(0, g).start()
    give(0, aligned)
    for k in range(1, levels):
        for g in range(2):
            across(k, g).start()
    for load in loads[3:7]:
        load.wait()
    ql = ql_ref[...]
    mine_l[...] = dot(ql, tok_ref[...], ((1,), (1,))).astype(bf16)
    give(1, aligned)
    mine_o[...] = ol_ref[...]
    scaled = (or_ref[...].astype(f32) * factor).astype(bf16)
    for q in range(n_pop):
        mine_a[q] = ql[:, q * cols:(q + 1) * cols]
        mine_b[q] = scaled[:, q * cols:(q + 1) * cols]
    give(2, aligned)
    give(3, aligned)
    packs_b[me] = mine_b[me]
    packs_a[me] = mine_a[me]
    packs_l[me] = mine_l[...]
    packs_q[me] = mine_q[...]
    packs_o[me] = mine_o[...]

    for load in loads[7:11]:
        load.wait()
    pair = dot(tok_ref[...], kv_ref[...])
    key = pair[:, :HEAD_DIM]
    key = (key * cos_ref[...] + pltpu.roll(key, HEAD_DIM // 2, 1) * sin_ref[...]).astype(bf16)
    values[:HEAD_DIM] = pair[:, HEAD_DIM:].T.astype(bf16)
    values[HEAD_DIM:] = jnp.ones((values.shape[0] - HEAD_DIM, tok), bf16)
    relay(0)
    give(0, crossed)
    give(1, crossed)
    spot = lax.broadcasted_iota(jnp.int32, (tok, HEAD_DIM), 0)
    lane = lax.broadcasted_iota(jnp.int32, (tok, HEAD_DIM), 1)
    for q in range(n_pop):
        keys[q, :, :HEAD_DIM] = key
        hidden = (spot > q * own_tok + lane) & (lane < own_tok)
        keys[q, :, HEAD_DIM:] = jnp.where(hidden, -1e30, 0.0).astype(bf16)
    relay(1)

    loads[11].wait()
    owner = me // (n_pop // n_mp)
    tgt = jnp.where(odd, tgt_ref[:, cols:], tgt_ref[:, :cols])
    goal[...] = jnp.where(mc == owner, -tgt, jnp.zeros_like(tgt))

    row_tok = lax.rem(lax.broadcasted_iota(jnp.int32, (own_tok, rows), 1), own_tok)
    pick_tok = (row_tok == lax.broadcasted_iota(jnp.int32, (own_tok, rows), 0)).astype(bf16)
    row_member = lax.broadcasted_iota(jnp.int32, (ranks, rows), 1) // own_tok
    same = row_member == lax.broadcasted_iota(jnp.int32, (ranks, rows), 0) // RANK

    def stacked(parts, *more):
        return jnp.concatenate(
            [p[i].astype(f32) for i in range(n_pop) for p in (parts,) + more], axis=0
        ).astype(bf16)

    filler = jnp.zeros((keys.shape[2] - HEAD_DIM - own_tok, rows), bf16)
    for slot in range(2):
        for h in range(heads):
            queries[slot, h, HEAD_DIM:HEAD_DIM + own_tok] = pick_tok
            queries[slot, h, HEAD_DIM + own_tok:] = filler
    total[...] = jnp.zeros_like(total)
    for k in range(2, levels - 1):
        relay(k)
    relay(levels - 1)
    packs_done(0).wait_recv()
    packs_done(1).wait_recv()
    pack_q = stacked(packs_q)
    low_all = stacked(packs_l)
    spot = lax.broadcasted_iota(jnp.int32, (tok, rows), 0)
    at_tok = lax.rem(lax.broadcasted_iota(jnp.int32, (tok, rows), 1), own_tok)
    for q in range(n_pop):
        sel = (spot == at_tok + q * own_tok).astype(bf16)
        low_rows[q] = jnp.where(same, dot(low_all, sel), 0.0).astype(bf16)

    def share(at, other):
        return pltpu.make_async_remote_copy(
            src_ref=known.at[at], dst_ref=known.at[at],
            send_sem=known_send, recv_sem=known_recv.at[at],
            device_id={"pop": other}, device_id_type=MESH,
        )

    loads[12].wait()
    loads[13].wait()
    all_of(along_in.at[:levels - 1], along_send, along_recv).wait_recv()
    own = own_base[...]
    for k in range(levels - 1):
        own = own + along_in[fars[k]].astype(f32)
    known[me] = own.astype(LINK)
    share(me, beside).start()
    share(me, 2 * nears[0] + side).start()
    give(2, crossed)
    give(3, crossed)
    for near in nears[1:]:
        share(me, 2 * near + side).start()

    scale = HEAD_DIM ** (-0.5) * math.log2(math.e)
    half = HEAD_DIM // 2
    def attend(group, first=0):
        for slot, at in enumerate(group):
            cosine = jnp.concatenate([cos_rows[at]] * (rows // 128), axis=1)
            sine = jnp.concatenate([sin_rows[at]] * (rows // 128), axis=1)
            mix = jnp.concatenate([pick_tok, low_rows[at]], axis=0)
            q_all = dot(jnp.concatenate([known[at], pack_q], axis=0), mix, ((0,), (0,)))
            for h in range(heads):
                low = q_all[h * HEAD_DIM:h * HEAD_DIM + half]
                high = q_all[h * HEAD_DIM + half:(h + 1) * HEAD_DIM]
                queries[slot, h, :half] = (low * cosine - high * sine).astype(bf16)
                queries[slot, h, half:HEAD_DIM] = (high * cosine + low * sine).astype(bf16)
        for slot, at in enumerate(group):
            for h in range(heads):
                s = dot(keys[at], queries[slot, h])
                scores[slot, h] = s
                peak = s[:8]
                for i in range(8, tok, 8):
                    peak = jnp.maximum(peak, s[i:i + 8])
                peaks[slot, h] = peak
        for slot, at in enumerate(group):
            for h in range(heads):
                peak = jnp.max(peaks[slot, h], axis=0, keepdims=True)
                exps[slot, h] = jnp.exp2((scores[slot, h] - peak) * scale).astype(bf16)
        for slot, at in enumerate(group):
            for h in range(heads):
                out = dot(values[...], exps[slot, h])
                inverse = 1.0 / out[HEAD_DIM:HEAD_DIM + 1]
                mixed[first + slot, h * HEAD_DIM:(h + 1) * HEAD_DIM] = (
                    out[:HEAD_DIM] * inverse
                ).astype(bf16)

    def near_copy(at):
        return pltpu.make_async_remote_copy(
            src_ref=terms.at[at, 1 - lax.rem(mc, 2)], dst_ref=near_in.at[at],
            send_sem=near_send, recv_sem=near_recv.at[at],
            device_id={"mp": near_mp}, device_id_type=MESH,
        )

    def far_copy(at):
        return pltpu.make_async_remote_copy(
            src_ref=far_out.at[at], dst_ref=far_in.at[at],
            send_sem=far_send, recv_sem=far_recv.at[at],
            device_id={"mp": far_mp}, device_id_type=MESH,
        )

    def project(group, slots):
        lows = [jnp.where(same, dot(wo_ref[cols:], mixed[slot]), 0.0) for slot in slots]
        for slot, at, low in zip(slots, group, lows):
            place = pl.ds(pl.multiple_of(at * own_tok, own_tok), own_tok)
            more = jnp.concatenate([right_o, right_o, right_o, goal[place, :]], axis=0)
            low = jnp.concatenate([*split3(low), pick_tok], axis=0)
            y = dot(wo_ref[:cols], mixed[slot]) + dot(more, low, ((0,), (0,)))
            terms[at] = y.reshape(terms.shape[1:]).astype(bf16)
        for at in group:
            near_copy(at).start()

    def join(at):
        near_copy(at).wait_recv()
        core, side = lax.rem(mc, 2), mc // 2
        own_sum[at] = terms[at, core, side].astype(f32) + near_in[at, side].astype(f32)
        far_out[at] = (
            terms[at, core, 1 - side].astype(f32) + near_in[at, 1 - side].astype(f32)
        ).astype(bf16)
        far_copy(at).start()

    def squares(at):
        far_copy(at).wait_recv()
        out = own_sum[at] + far_in[at].astype(f32)
        out = out * out
        more = total[...]
        for i in range(quarter // 8):
            more = more + out[i * 8:(i + 1) * 8]
        total[...] = more

    attend((me,), 2)

    def expect(at, pass_on):
        share(at, beside).wait_recv()
        if pass_on:
            share(at, beside).start()

    column = [2 * near + side for near in nears]
    beyond = [2 * near + 1 - side for near in nears]
    groups = [(me,), (beside, column[0])]
    for i in range(1, levels - 1):
        groups.append((column[i], beyond[i - 1]))
    groups.append((beyond[levels - 2],))
    expect(beside, False)
    expect(column[0], True)
    attend(groups[1])
    packs_done(2).wait_recv()
    packs_done(3).wait_recv()
    right_o = jnp.concatenate(
        [packs_b[i].astype(f32) for i in range(n_pop)], axis=0
    ).astype(bf16)
    loads[14].wait()
    pack_o = stacked(packs_o)
    wo_ref[cols:] = pack_o
    project(groups[0] + groups[1], (2, 0, 1))
    give(4, aligned + crossed)
    expect(column[1], True)
    groups = [groups[0] + groups[1]] + groups[2:]
    for k in range(1, len(groups)):
        expect(beyond[k - 1], False)
        attend(groups[k])
        if k + 1 < levels - 1:
            expect(column[k + 1], True)
        for at in groups[k - 1]:
            join(at)
        project(groups[k], range(len(groups[k])))
    for at in groups[0]:
        squares(at)
    for at in groups[-1]:
        join(at)
    for group in groups[1:]:
        for at in group:
            squares(at)

    lane_row = lax.broadcasted_iota(jnp.int32, (1, 128), 1)
    sums = jnp.sum(total[...], axis=0, keepdims=True)
    member_of = lax.broadcasted_iota(jnp.int32, (1, rows), 1) // own_tok
    mine = jnp.zeros((1, 128), f32)
    for k in range(n_pop):
        value_k = jnp.sum(jnp.where(member_of == k, sums, 0.0), axis=1, keepdims=True)
        mine = mine + jnp.where(lane_row == k, value_k, 0.0)

    my_id = mc * n_pop + me
    errs[my_id] = mine

    for p, m in others:
        pltpu.make_async_remote_copy(
            src_ref=errs.at[my_id], dst_ref=errs.at[my_id], send_sem=err_send, recv_sem=err_recv,
            device_id={"pop": p, "mp": m}, device_id_type=MESH,
        ).start()
    all_errs = all_of(errs.at[:n_dev - 1], err_send, err_recv)
    for kind in range(len(gathered)):
        packs_done(kind).wait_send()
    all_of(part.at[0], across_send, across_recv.at[0, 0]).wait_send()
    all_of(along_out.at[:levels - 1], along_send, along_recv).wait_send()
    all_of(known.at[:n_pop - 1], known_send, known_recv.at[0]).wait_send()
    all_of(near_in, near_send, near_recv.at[0]).wait_send()
    all_of(far_in, far_send, far_recv.at[0]).wait_send()
    rows_out[0] = pack_q
    rows_out[1] = pack_o
    packs_done(4).wait_recv()
    for i, packs in enumerate((packs_a, packs_b)):
        some = jnp.concatenate([packs[j].astype(f32) for j in range(n_pop)], axis=0)
        some = jnp.concatenate([some] * 3 + [jnp.zeros((left_out.shape[2] - 3 * ranks, cols), f32)], axis=0)
        some = jnp.concatenate(
            [some, jnp.zeros((some.shape[0], left_out.shape[1] - cols), f32)], axis=1
        )
        left_out[i] = some.T.astype(bf16)
    all_errs.wait_recv()
    error = errs[0]
    for i in range(1, n_dev):
        error = error + errs[i]
    live = lane_row < n_pop
    fitness = -(error / (tok * width))
    mean = jnp.sum(jnp.where(live, fitness, 0.0), axis=1, keepdims=True) / n_pop
    dev = jnp.where(live, fitness - mean, 0.0)
    spread = jnp.sum(dev * dev, axis=1, keepdims=True) / n_pop
    weight = dev / jnp.sqrt(spread + spread_floor)
    stat_out[...] = jnp.concatenate(
        [fitness, weight, jnp.zeros((6, 128), f32)], axis=0
    )

    all_errs.wait_send()


def grad_kernel(rows_ref, left_ref, stat_ref, gq_hbm, got_hbm, fit_hbm, gq_ref, got_ref, fit_ref, sem, fit_sem):
    ranks, feats = rows_ref.shape[1:]
    cols = gq_ref.shape[0]
    row = lax.broadcasted_iota(jnp.int32, (ranks, 128), 0)
    lane = lax.broadcasted_iota(jnp.int32, (ranks, 128), 1)
    weight = jnp.sum(jnp.where(lane == row // RANK, stat_ref[1:2, :], 0.0), axis=1, keepdims=True)
    weight = weight / (noise_scale * noise_scale)
    filler = jnp.zeros((left_ref.shape[2] - 3 * ranks, feats), bf16)
    step = cols // (sem.shape[0] // 2)
    copies = []
    for i, (out, target) in enumerate(((gq_ref, gq_hbm), (got_ref, got_hbm))):
        right = jnp.concatenate([*split3(rows_ref[i].astype(f32) * weight), filler], axis=0)
        for low in range(0, cols, step):
            out[low:low + step, :] = dot(left_ref[i, low:low + step, :], right)
            copy = pltpu.make_async_copy(
                out.at[low:low + step], target.at[low:low + step], sem.at[len(copies)]
            )
            copy.start()
            copies.append(copy)
    me = lax.axis_index("pop")
    fit_ref[0] = jnp.sum(jnp.where(lane[:1] == me, stat_ref[0:1, :], 0.0))
    copy = pltpu.make_async_copy(fit_ref, fit_hbm, fit_sem)
    copy.start()
    copies.append(copy)
    for copy in copies:
        copy.wait()


def per_device_fast(
    n_pop, n_mp,
    tokens, target, w_query, w_key, w_value, w_out,
    query_left_factors, query_right_factors, o_left, o_right, member_ids,
):
    tok, width = tokens.shape
    feats = w_query.shape[1]
    cols = w_out.shape[1]
    own_tok = tok // n_pop
    rows = n_pop * own_tok
    cosine, sine = rope_tables(tok, HEAD_DIM)
    half = HEAD_DIM // 2
    by_row = lambda x: np.tile(
        x[:, half:].T.reshape(half, n_pop, own_tok).transpose(1, 0, 2), (1, 1, 128 // own_tok)
    )
    vmem = pl.BlockSpec(memory_space=pltpu.VMEM)
    hbm = pl.BlockSpec(memory_space=pltpu.HBM)
    dma = pltpu.SemaphoreType.DMA
    n_dev = n_pop * n_mp
    like = lambda x: pltpu.VMEM(x.shape, x.dtype)
    wot = w_out.T
    packs, left, stat = pl.pallas_call(
        functools.partial(forward_kernel, n_pop, n_mp, width),
        name="forward",
        out_shape=(
            pltpu.VMEM((2, n_pop * RANK, feats), bf16),
            pltpu.VMEM((2, -(-cols // 128) * 128, n_pop * PACK * 2), bf16),
            pltpu.VMEM((8, 128), f32),
        ),
        in_specs=[hbm] * 15,
        out_specs=(vmem, vmem, vmem),
        scratch_shapes=[
            pltpu.SMEM((1,), jnp.int32), pltpu.VMEM((tok, cols + cols % 128), bf16), pltpu.VMEM((cols + cols % 128, feats), bf16), pltpu.VMEM((RANK, feats), bf16),
            like(tokens), pltpu.VMEM((RANK, width), bf16),
            pltpu.VMEM((RANK, feats), bf16), pltpu.VMEM((RANK, width), bf16),
            pltpu.VMEM((width, 2 * HEAD_DIM), bf16),
            pltpu.VMEM((tok, HEAD_DIM), f32), pltpu.VMEM((tok, HEAD_DIM), f32), like(target),
            pltpu.VMEM((n_pop, HEAD_DIM // 2, 128), f32),
            pltpu.VMEM((n_pop, HEAD_DIM // 2, 128), f32),
            pltpu.VMEM((cols + n_pop * RANK, feats), bf16),
            pltpu.VMEM((2, n_pop // 2, own_tok, feats), LINK),
            pltpu.VMEM((n_pop // 2, own_tok, feats), LINK),
            pltpu.VMEM((n_pop // 2, own_tok, feats), LINK),
            pltpu.VMEM((n_pop // 2, own_tok, feats), LINK),
            pltpu.VMEM((own_tok, feats), f32),
            pltpu.VMEM((n_pop, own_tok, feats), LINK),
            pltpu.VMEM((RANK, tok), bf16),
            pltpu.VMEM((n_pop, RANK, tok), bf16),
            pltpu.VMEM((RANK, feats), bf16),
            pltpu.VMEM((n_pop, RANK, feats), bf16),
            pltpu.VMEM((RANK, feats), bf16),
            pltpu.VMEM((n_pop, RANK, feats), bf16),
            pltpu.VMEM((n_pop, RANK, cols), bf16),
            pltpu.VMEM((n_pop, RANK, cols), bf16),
            pltpu.VMEM((n_pop, RANK, cols), bf16),
            pltpu.VMEM((n_pop, RANK, cols), bf16),
            pltpu.VMEM((n_pop, tok, 2 * HEAD_DIM), bf16),
            pltpu.VMEM((HEAD_DIM + 16, tok), bf16),
            pltpu.VMEM((n_pop, n_pop * RANK, rows), bf16),
            pltpu.VMEM((tok, cols), bf16),
            pltpu.VMEM((2, feats // HEAD_DIM, 2 * HEAD_DIM, rows), bf16),
            pltpu.VMEM((2, feats // HEAD_DIM, tok, rows), f32),
            pltpu.VMEM((2, feats // HEAD_DIM, 8, rows), f32),
            pltpu.VMEM((2, feats // HEAD_DIM, tok, rows), bf16),
            pltpu.VMEM((3, feats, rows), bf16),
            pltpu.VMEM((n_pop, 2, n_mp // 2, cols // n_mp, rows), bf16),
            pltpu.VMEM((n_pop, n_mp // 2, cols // n_mp, rows), bf16),
            pltpu.VMEM((n_pop, cols // n_mp, rows), bf16),
            pltpu.VMEM((n_pop, cols // n_mp, rows), bf16),
            pltpu.VMEM((n_pop, cols // n_mp, rows), f32),
            pltpu.VMEM((8, rows), f32),
            pltpu.VMEM((n_dev, 1, 128), f32),
            dma((16,)),
            dma, dma((n_pop // 2, 2)), dma, dma,
            dma((5,)), dma((5,)), dma, dma((n_pop,)),
            dma, dma((n_pop,)), dma, dma((n_pop,)),
            dma, dma,
        ],
        compiler_params=pltpu.CompilerParams(
            collective_id=0, has_side_effects=True, vmem_limit_bytes=60 * 1024 * 1024
        ),
    )(tokens, w_query, w_key, w_value, wot, target,
      query_left_factors[0].T, query_right_factors[0], o_left[0].T, o_right[0],
      jnp.asarray(cosine), jnp.asarray(sine), jnp.asarray(by_row(cosine)), jnp.asarray(by_row(sine)),
      member_ids)
    grad = jax.ShapeDtypeStruct((cols, feats), f32)
    grad_query, grad_out_t, fitness = pl.pallas_call(
        grad_kernel,
        name="grads",
        out_shape=(grad, grad, jax.ShapeDtypeStruct((1,), f32)),
        in_specs=[vmem, vmem, vmem],
        out_specs=(hbm, hbm, hbm),
        scratch_shapes=[like(grad), like(grad), pltpu.SMEM((1,), f32), dma((8,)), dma],
        compiler_params=pltpu.CompilerParams(vmem_limit_bytes=16 * 1024 * 1024),
    )(packs, left, stat)
    return grad_query, grad_out_t.T, fitness


def tables(count, head_size):
    position = jnp.arange(count, dtype=jnp.float32)
    index = jnp.arange(head_size // 2, dtype=jnp.float32)
    freq = jnp.exp(-math.log(rope_base) * 2.0 * index / head_size)
    angle = position[:, None] * freq[None, :]
    return (jnp.cos(angle)[:, None, :], jnp.sin(angle)[:, None, :])


def rotate(field, cosine_table, sine):
    half = field.shape[-1] // 2
    first = field[..., :half]
    second = field[..., half:]
    return jnp.concatenate(
        [first * cosine_table - second * sine, second * cosine_table + first * sine], axis=-1
    )


def per_device(
    tokens,
    target,
    w_query,
    w_key,
    w_value,
    w_out,
    query_left_factors,
    query_right_factors,
    o_left,
    o_right,
    member_ids,
):
    tok = tokens.shape[0]
    local_feats = w_query.shape[1]
    local_kv = w_key.shape[1] // HEAD_DIM
    group = group_of(w_query, w_key)
    local_heads = local_kv * group
    slots = query_left_factors.shape[0]
    scale = HEAD_DIM ** (-0.5)
    cosine_table, sine = tables(tok, HEAD_DIM)
    base = jnp.dot(
        tokens,
        lax.all_gather(w_query, "pop", axis=0, tiled=True),
        preferred_element_type=jnp.float32,
    )
    keys = rotate(
        jnp.dot(tokens, w_key, preferred_element_type=jnp.float32).reshape(tok, local_kv, HEAD_DIM),
        cosine_table,
        sine,
    ).astype(jnp.bfloat16)
    values = (
        jnp.dot(tokens, w_value, preferred_element_type=jnp.float32)
        .astype(jnp.bfloat16)
        .reshape(tok, local_kv, HEAD_DIM)
    )
    signs = (1 - 2 * (member_ids % 2)).astype(jnp.float32)
    factor = noise_scale * signs[:, None, None]
    lowrank_product = jnp.einsum(
        "td,mdr->mtr", tokens, query_left_factors, preferred_element_type=jnp.float32
    ).astype(jnp.bfloat16)
    query = base[None] + factor * jnp.einsum(
        "olj,ojv->olv", lowrank_product, query_right_factors, preferred_element_type=jnp.float32
    )
    query = rotate(
        query.reshape(slots, tok, local_heads, HEAD_DIM), cosine_table[None], sine[None]
    ).astype(jnp.bfloat16)
    query = query.reshape(slots, tok, local_kv, group, HEAD_DIM)
    scores = jnp.einsum("mtkgd,skd->mkgts", query, keys, preferred_element_type=jnp.float32) * scale
    causal = jnp.arange(tok)[:, None] >= jnp.arange(tok)[None, :]
    scores = jnp.where(causal, scores, -1e30)
    probs = jax.nn.softmax(scores, axis=-1).astype(jnp.bfloat16)
    mixed = (
        jnp.einsum("mkgts,skd->mtkgd", probs, values, preferred_element_type=jnp.float32)
        .astype(jnp.bfloat16)
        .reshape(slots, tok, local_feats)
    )
    low_out = jnp.einsum("mtf,mfr->mtr", mixed, o_left, preferred_element_type=jnp.float32)
    right_full = o_right.astype(jnp.float32)
    part = jnp.einsum(
        "mtf,fe->mte",
        mixed,
        lax.all_gather(w_out, "pop", axis=1, tiled=True),
        preferred_element_type=jnp.float32,
    )
    term = part + factor * jnp.einsum(
        "mtr,mre->mte", low_out, right_full, precision=lax.Precision.HIGHEST
    )
    output = lax.psum_scatter(
        term.astype(jnp.bfloat16), "mp", scatter_dimension=2, tiled=True
    ).astype(jnp.float32)
    diff = output - target.astype(jnp.float32)[None]
    errors = lax.psum(jnp.sum(diff * diff, axis=(1, 2)), "mp")
    fitness = -(errors / (tok * tokens.shape[1]))
    count = slots * lax.axis_size("pop")
    mean = lax.psum(jnp.sum(fitness), "pop") / count
    spread = lax.psum(jnp.sum((fitness - mean) * (fitness - mean)), "pop") / count
    weight = signs * (fitness - mean) / jnp.sqrt(spread + spread_floor)
    every_weight = lax.all_gather(weight, "pop", axis=0, tiled=True)
    right_factors_gathered, left_all = (
        lax.all_gather(query_right_factors, "pop", axis=0, tiled=True),
        lax.all_gather(o_left, "pop", axis=0, tiled=True),
    )
    rows_q = lax.all_to_all(query_left_factors, "pop", split_axis=1, concat_axis=0, tiled=True)
    cols_o = lax.all_to_all(o_right, "pop", split_axis=2, concat_axis=0, tiled=True)
    whole_population = rows_q.shape[0]
    left_q = jnp.transpose(
        rows_q.astype(jnp.float32) * every_weight[:, None, None], (1, 0, 2)
    ).reshape(rows_q.shape[1], whole_population * RANK)
    right_q = right_factors_gathered.astype(jnp.float32).reshape(
        whole_population * RANK, local_feats
    )
    grad_query = jnp.dot(left_q, right_q, precision=lax.Precision.HIGHEST) / noise_scale
    output_left_factor = jnp.transpose(
        left_all.astype(jnp.float32) * every_weight[:, None, None], (1, 0, 2)
    ).reshape(local_feats, whole_population * RANK)
    right_o = cols_o.astype(jnp.float32).reshape(whole_population * RANK, cols_o.shape[2])
    grad_out = jnp.dot(output_left_factor, right_o, precision=lax.Precision.HIGHEST) / noise_scale
    return (grad_query, grad_out, fitness)


def group_of(w_query, w_key):
    return w_query.shape[1] // w_key.shape[1]


def pick(args, n_pop, n_mp):
    tok = args[0].shape[0]
    kernel = (
        args[6].shape[0] == n_pop
        and n_mp == 4
        and n_pop % n_mp == 0
        and n_pop % 2 == 0
        and n_pop * PACK <= 128
        and tok % (n_pop * 16) == 0
        and tok // n_pop < 128
        and 128 % (tok // n_pop) == 0
        and args[5].shape[1] // n_pop % (16 * n_mp) == 0
        and n_pop >= 8
        and n_pop * PACK * 2 % 128 == 0
        and args[2].shape[1] // n_mp == 2 * args[5].shape[1] // n_pop
        and args[2].shape[0] == args[5].shape[1]
        and args[3].shape[1] == n_mp * HEAD_DIM
    )
    return functools.partial(per_device_fast, n_pop, n_mp) if kernel else per_device


def solution(mesh):
    placed = (
        P(),
        P(None, "mp"),
        P("pop", "mp"),
        P(None, "mp"),
        P(None, "mp"),
        P("mp", "pop"),
        P("pop", None, None),
        P("pop", None, "mp"),
        P("pop", "mp", None),
        P("pop", None, None),
        P("pop"),
    )
    n_pop, n_mp = mesh.shape["pop"], mesh.shape["mp"]

    def whole(*args):
        return jax.shard_map(
            pick(args, n_pop, n_mp),
            mesh=mesh,
            in_specs=placed,
            out_specs=(P("pop", "mp"), P("mp", "pop"), P("pop")),
            check_vma=False,
        )(*args)

    return whole
```

```python
import functools
import math

import jax
import jax.numpy as jnp
import numpy as np
from jax import lax
from jax.experimental import pallas as pl
from jax.experimental.pallas import tpu as pltpu
from jax.sharding import PartitionSpec as P

HEAD_DIM = 128
RANK = 4
PACK = 8
LINK = jnp.bfloat16

noise_scale = 0.5
rope_base = 1000000.0
spread_floor = 0.001
MESH = pl.DeviceIdType.MESH
f32 = jnp.float32
bf16 = jnp.bfloat16


def rope_tables(count, head_size):
    index = np.arange(head_size // 2, dtype=np.float64)
    freq = np.exp(-math.log(rope_base) * 2.0 * index / head_size)
    angle = np.arange(count, dtype=np.float64)[:, None] * freq[None, :]
    cosine, sine = np.cos(angle), np.sin(angle)
    return (
        np.concatenate([cosine, cosine], 1).astype(np.float32),
        np.concatenate([-sine, sine], 1).astype(np.float32),
    )


def dot(a, b, dims=((1,), (0,))):
    return lax.dot_general(a, b, (dims, ((), ())), preferred_element_type=f32)


def split3(x):
    hi = x.astype(bf16)
    rest = x - hi.astype(f32)
    mid = rest.astype(bf16)
    low = (rest - mid.astype(f32)).astype(bf16)
    return hi, mid, low


def forward_kernel(
    n_pop, n_mp, width,
    tok_hbm, wq_hbm, wk_hbm, wv_hbm, wo_hbm, tgt_hbm, ql_hbm, qr_hbm, ol_hbm, or_hbm,
    cos_hbm, sin_hbm, cos_rows_hbm, sin_rows_hbm, id_hbm,
    rows_out, left_out, stat_out,
    id_ref, window, wq_ref, qr_ref, tok_ref, ql_ref, ol_ref, or_ref, kv_ref, cos_ref, sin_ref,
    tgt_ref, cos_rows, sin_rows, wo_ref,
    part, across_in, along_out, along_in, own_base, known, mine_l, packs_l, mine_q, packs_q,
    mine_o, packs_o, mine_b, packs_b, mine_a, packs_a,
    keys, values, low_rows, goal, queries, scores, peaks, exps, mixed, terms, near_in, far_out, far_in, own_sum, total, errs,
    load_sem, heard, across_send, across_recv, along_send, along_recv,
    pop_send, pop_recv, known_send, known_recv, near_send, near_recv, far_send, far_recv, err_send, err_recv,
):
    me = lax.axis_index("pop")
    mc = lax.axis_index("mp")
    n_dev = n_pop * n_mp
    tok, feats = tok_ref.shape[0], wq_ref.shape[1]
    own_tok = tok // n_pop
    rows = n_pop * own_tok
    heads = feats // HEAD_DIM
    cols = wo_hbm.shape[0]
    ranks = n_pop * RANK
    quarter = cols // n_mp
    odd = lax.rem(me, 2) == 1
    lead = wq_ref.shape[0] - cols
    near_cols = pl.ds(pl.multiple_of(me * cols - jnp.where(odd, lead, 0), 128), cols + lead)
    near_rows = pl.ds(pl.multiple_of(jnp.where(odd, lead, 0), 16), cols)
    loads = [
        pltpu.make_async_copy(src, dst, load_sem.at[i])
        for i, (src, dst) in enumerate((
            (tok_hbm.at[:, near_cols], window), (wq_hbm, wq_ref.at[near_rows]), (qr_hbm, qr_ref),
            (tok_hbm, tok_ref), (ql_hbm, ql_ref), (ol_hbm, ol_ref), (or_hbm, or_ref),
            (wk_hbm, kv_ref.at[:, :HEAD_DIM]), (wv_hbm, kv_ref.at[:, HEAD_DIM:]),
            (cos_hbm, cos_ref), (sin_hbm, sin_ref), (tgt_hbm, tgt_ref),
            (cos_rows_hbm, cos_rows), (sin_rows_hbm, sin_rows), (wo_hbm, wo_ref.at[:cols]),
            (id_hbm, id_ref),
        ))
    ]
    for load in loads[:3] + loads[15:]:
        load.start()

    barrier = pltpu.get_barrier_semaphore()

    pops = [lax.rem(me + i, n_pop) for i in range(n_pop)]
    mps = [lax.rem(mc + i, n_mp) for i in range(n_mp)]
    others = [(p, m) for m in mps for p in pops][1:]
    side, level = lax.rem(me, 2), me // 2
    levels = n_pop // 2
    beside = me + 1 - 2 * side
    aligned = [2 * lax.rem(level + i, levels) + side for i in range(1, levels)]
    near_mp, far_mp = mc + 1 - 2 * lax.rem(mc, 2), lax.rem(mc + 2, n_mp)
    partners = [(beside, mc), (me, near_mp), (me, far_mp)]

    def tell(semaphore, p, m=mc):
        pl.semaphore_signal(
            semaphore, inc=1, device_id={"pop": p, "mp": m}, device_id_type=MESH
        )

    def tell_neighbours(semaphore):
        @pl.when(level > 0)
        def _():
            tell(semaphore, me - 2)

        @pl.when(level < levels - 1)
        def _():
            tell(semaphore, me + 2)

    neighbours = jnp.where(level > 0, 1, 0) + jnp.where(level < levels - 1, 1, 0)
    tell_neighbours(barrier)
    for p, m in partners:
        tell(barrier, p, m)

    if lead:
        wq_ref[pl.ds(pl.multiple_of(jnp.where(odd, 0, cols), 16), lead), :] = jnp.zeros(
            (lead, feats), bf16
        )
    for load in loads[3:15]:
        load.start()
    for load in loads[:3] + loads[15:]:
        load.wait()
    sign = 1 - 2 * lax.rem(id_ref[0], 2)
    factor = noise_scale * sign.astype(f32)
    base = dot(window[...], wq_ref[...])
    for b in range(n_pop):
        part[b % 2, b // 2] = base[b * own_tok:(b + 1) * own_tok].astype(LINK)
    mine_q[...] = (qr_ref[...].astype(f32) * factor).astype(bf16)

    pl.semaphore_wait(barrier, len(partners) + neighbours)
    tell_neighbours(heard.at[0])

    ways = [
        sorted(range(levels), key=lambda t: (-abs(t - u), (t < levels // 2) == (u < levels // 2)))
        for u in range(levels)
    ]

    def far(k):
        at = jnp.int32(ways[0][k])
        for u in range(1, levels):
            at = jnp.where(level == u, ways[u][k], at)
        return at

    fars = [far(k) for k in range(levels)]
    nears = fars[:-1][::-1]

    cut = (heads + 1) // 2 * HEAD_DIM
    halves = (slice(0, cut), slice(cut, feats))

    def across(k, g):
        return pltpu.make_async_remote_copy(
            src_ref=part.at[1 - side, fars[k], :, halves[g]],
            dst_ref=across_in.at[fars[k], :, halves[g]],
            send_sem=across_send, recv_sem=across_recv.at[k, g],
            device_id={"pop": beside}, device_id_type=MESH,
        )

    def along(k, g):
        return pltpu.make_async_remote_copy(
            src_ref=along_out.at[fars[k], :, halves[g]],
            dst_ref=along_in.at[level, :, halves[g]],
            send_sem=along_send, recv_sem=along_recv,
            device_id={"pop": 2 * fars[k] + side}, device_id_type=MESH,
        )

    def relay(k):
        for g, lanes in enumerate(halves):
            across(k, g).wait_recv()
            joined = part[side, fars[k], :, lanes].astype(f32)
            joined = joined + across_in[fars[k], :, lanes].astype(f32)
            if k == levels - 1:
                own_base[:, lanes] = joined
            else:
                along_out[fars[k], :, lanes] = joined.astype(LINK)
                along(k, g).start()

    gathered = ((mine_q, packs_q), (mine_l, packs_l), (mine_o, packs_o), (mine_b, packs_b),
                (mine_a, packs_a))

    crossed = [2 * lax.rem(level + i, levels) + 1 - side for i in range(levels)]

    def give(kind, places):
        mine, packs = gathered[kind]
        for other in places:
            pltpu.make_async_remote_copy(
                src_ref=mine.at[other] if kind >= 3 else mine, dst_ref=packs.at[me],
                send_sem=pop_send.at[kind], recv_sem=pop_recv.at[kind],
                device_id={"pop": other}, device_id_type=MESH,
            ).start()

    def all_of(refs, send_sem, recv_sem):
        return pltpu.make_async_remote_copy(
            src_ref=refs, dst_ref=refs, send_sem=send_sem, recv_sem=recv_sem,
            device_id={"pop": beside}, device_id_type=MESH,
        )

    def packs_done(kind):
        return all_of(gathered[kind][1].at[:n_pop - 1], pop_send.at[kind], pop_recv.at[kind])

    for g in range(2):
        across(0, g).start()
    for k in range(1, levels):
        for g in range(2):
            across(k, g).start()
    for load in loads[3:7]:
        load.wait()
    ql = ql_ref[...]
    mine_l[...] = dot(ql, tok_ref[...], ((1,), (1,))).astype(bf16)
    for r in range(1, levels - 2):
        pl.semaphore_wait(heard.at[r - 1], neighbours)
        tell_neighbours(heard.at[r])
    mine_o[...] = ol_ref[...]
    scaled = (or_ref[...].astype(f32) * factor).astype(bf16)
    for q in range(n_pop):
        mine_a[q] = ql[:, q * cols:(q + 1) * cols]
        mine_b[q] = scaled[:, q * cols:(q + 1) * cols]
    packs_b[me] = mine_b[me]
    packs_a[me] = mine_a[me]
    packs_l[me] = mine_l[...]
    packs_q[me] = mine_q[...]
    packs_o[me] = mine_o[...]

    for load in loads[7:11]:
        load.wait()
    pair = dot(tok_ref[...], kv_ref[...])
    key = pair[:, :HEAD_DIM]
    key = (key * cos_ref[...] + pltpu.roll(key, HEAD_DIM // 2, 1) * sin_ref[...]).astype(bf16)
    values[:HEAD_DIM] = pair[:, HEAD_DIM:].T.astype(bf16)
    values[HEAD_DIM:] = jnp.ones((values.shape[0] - HEAD_DIM, tok), bf16)
    pl.semaphore_wait(heard.at[levels - 3], neighbours)
    tell(heard.at[levels - 2], beside)
    for kind in range(4):
        give(kind, aligned)
    relay(0)
    pl.semaphore_wait(heard.at[levels - 2], 1)
    give(0, crossed)
    give(1, crossed)
    spot = lax.broadcasted_iota(jnp.int32, (tok, HEAD_DIM), 0)
    lane = lax.broadcasted_iota(jnp.int32, (tok, HEAD_DIM), 1)
    for q in range(n_pop):
        keys[q, :, :HEAD_DIM] = key
        hidden = (spot > q * own_tok + lane) & (lane < own_tok)
        keys[q, :, HEAD_DIM:] = jnp.where(hidden, -1e30, 0.0).astype(bf16)
    relay(1)

    loads[11].wait()
    owner = me // (n_pop // n_mp)
    tgt = jnp.where(odd, tgt_ref[:, cols:], tgt_ref[:, :cols])
    goal[...] = jnp.where(mc == owner, -tgt, jnp.zeros_like(tgt))

    row_tok = lax.rem(lax.broadcasted_iota(jnp.int32, (own_tok, rows), 1), own_tok)
    pick_tok = (row_tok == lax.broadcasted_iota(jnp.int32, (own_tok, rows), 0)).astype(bf16)
    row_member = lax.broadcasted_iota(jnp.int32, (ranks, rows), 1) // own_tok
    same = row_member == lax.broadcasted_iota(jnp.int32, (ranks, rows), 0) // RANK

    def stacked(parts, *more):
        return jnp.concatenate(
            [p[i].astype(f32) for i in range(n_pop) for p in (parts,) + more], axis=0
        ).astype(bf16)

    filler = jnp.zeros((keys.shape[2] - HEAD_DIM - own_tok, rows), bf16)
    for slot in range(2):
        for h in range(heads):
            queries[slot, h, HEAD_DIM:HEAD_DIM + own_tok] = pick_tok
            queries[slot, h, HEAD_DIM + own_tok:] = filler
    total[...] = jnp.zeros_like(total)
    for k in range(2, levels - 1):
        relay(k)
    relay(levels - 1)
    packs_done(0).wait_recv()
    packs_done(1).wait_recv()
    pack_q = stacked(packs_q)
    low_all = stacked(packs_l)
    spot = lax.broadcasted_iota(jnp.int32, (tok, rows), 0)
    at_tok = lax.rem(lax.broadcasted_iota(jnp.int32, (tok, rows), 1), own_tok)
    for q in range(n_pop):
        sel = (spot == at_tok + q * own_tok).astype(bf16)
        low_rows[q] = jnp.where(same, dot(low_all, sel), 0.0).astype(bf16)

    def share(at, other):
        return pltpu.make_async_remote_copy(
            src_ref=known.at[at], dst_ref=known.at[at],
            send_sem=known_send, recv_sem=known_recv.at[at],
            device_id={"pop": other}, device_id_type=MESH,
        )

    loads[12].wait()
    loads[13].wait()
    all_of(along_in.at[:levels - 1], along_send, along_recv).wait_recv()
    own = own_base[...]
    for k in range(levels - 1):
        own = own + along_in[fars[k]].astype(f32)
    known[me] = own.astype(LINK)
    share(me, beside).start()
    share(me, 2 * nears[0] + side).start()
    give(2, crossed)
    give(3, crossed)
    for near in nears[1:]:
        share(me, 2 * near + side).start()

    scale = HEAD_DIM ** (-0.5) * math.log2(math.e)
    half = HEAD_DIM // 2
    def attend(group, first=0):
        for slot, at in enumerate(group):
            cosine = jnp.concatenate([cos_rows[at]] * (rows // 128), axis=1)
            sine = jnp.concatenate([sin_rows[at]] * (rows // 128), axis=1)
            mix = jnp.concatenate([pick_tok, low_rows[at]], axis=0)
            q_all = dot(jnp.concatenate([known[at], pack_q], axis=0), mix, ((0,), (0,)))
            for h in range(heads):
                low = q_all[h * HEAD_DIM:h * HEAD_DIM + half]
                high = q_all[h * HEAD_DIM + half:(h + 1) * HEAD_DIM]
                queries[slot, h, :half] = (low * cosine - high * sine).astype(bf16)
                queries[slot, h, half:HEAD_DIM] = (high * cosine + low * sine).astype(bf16)
        for slot, at in enumerate(group):
            for h in range(heads):
                s = dot(keys[at], queries[slot, h])
                scores[slot, h] = s
                peak = s[:8]
                for i in range(8, tok, 8):
                    peak = jnp.maximum(peak, s[i:i + 8])
                peaks[slot, h] = peak
        for slot, at in enumerate(group):
            for h in range(heads):
                peak = jnp.max(peaks[slot, h], axis=0, keepdims=True)
                exps[slot, h] = jnp.exp2((scores[slot, h] - peak) * scale).astype(bf16)
        for slot, at in enumerate(group):
            for h in range(heads):
                out = dot(values[...], exps[slot, h])
                inverse = 1.0 / out[HEAD_DIM:HEAD_DIM + 1]
                mixed[first + slot, h * HEAD_DIM:(h + 1) * HEAD_DIM] = (
                    out[:HEAD_DIM] * inverse
                ).astype(bf16)

    def near_copy(at):
        return pltpu.make_async_remote_copy(
            src_ref=terms.at[at, 1 - lax.rem(mc, 2)], dst_ref=near_in.at[at],
            send_sem=near_send, recv_sem=near_recv.at[at],
            device_id={"mp": near_mp}, device_id_type=MESH,
        )

    def far_copy(at):
        return pltpu.make_async_remote_copy(
            src_ref=far_out.at[at], dst_ref=far_in.at[at],
            send_sem=far_send, recv_sem=far_recv.at[at],
            device_id={"mp": far_mp}, device_id_type=MESH,
        )

    def project(group, slots):
        lows = [jnp.where(same, dot(wo_ref[cols:], mixed[slot]), 0.0) for slot in slots]
        for slot, at, low in zip(slots, group, lows):
            place = pl.ds(pl.multiple_of(at * own_tok, own_tok), own_tok)
            more = jnp.concatenate([right_o, right_o, right_o, goal[place, :]], axis=0)
            low = jnp.concatenate([*split3(low), pick_tok], axis=0)
            y = dot(wo_ref[:cols], mixed[slot]) + dot(more, low, ((0,), (0,)))
            terms[at] = y.reshape(terms.shape[1:]).astype(bf16)
        for at in group:
            near_copy(at).start()

    def join(at):
        near_copy(at).wait_recv()
        core, side = lax.rem(mc, 2), mc // 2
        own_sum[at] = terms[at, core, side].astype(f32) + near_in[at, side].astype(f32)
        far_out[at] = (
            terms[at, core, 1 - side].astype(f32) + near_in[at, 1 - side].astype(f32)
        ).astype(bf16)
        far_copy(at).start()

    def squares(at):
        far_copy(at).wait_recv()
        out = own_sum[at] + far_in[at].astype(f32)
        out = out * out
        more = total[...]
        for i in range(quarter // 8):
            more = more + out[i * 8:(i + 1) * 8]
        total[...] = more

    attend((me,), 2)

    def expect(at, pass_on):
        share(at, beside).wait_recv()
        if pass_on:
            share(at, beside).start()

    column = [2 * near + side for near in nears]
    beyond = [2 * near + 1 - side for near in nears]
    groups = [(me,), (beside, column[0])]
    for i in range(1, levels - 1):
        groups.append((column[i], beyond[i - 1]))
    groups.append((beyond[levels - 2],))
    expect(beside, False)
    expect(column[0], True)
    attend(groups[1])
    packs_done(2).wait_recv()
    packs_done(3).wait_recv()
    right_o = jnp.concatenate(
        [packs_b[i].astype(f32) for i in range(n_pop)], axis=0
    ).astype(bf16)
    loads[14].wait()
    pack_o = stacked(packs_o)
    wo_ref[cols:] = pack_o
    project(groups[0] + groups[1], (2, 0, 1))
    give(4, aligned + crossed)
    expect(column[1], True)
    groups = [groups[0] + groups[1]] + groups[2:]
    for k in range(1, len(groups)):
        expect(beyond[k - 1], False)
        attend(groups[k])
        if k + 1 < levels - 1:
            expect(column[k + 1], True)
        for at in groups[k - 1]:
            join(at)
        project(groups[k], range(len(groups[k])))
    for at in groups[0]:
        squares(at)
    for at in groups[-1]:
        join(at)
    for group in groups[1:]:
        for at in group:
            squares(at)

    lane_row = lax.broadcasted_iota(jnp.int32, (1, 128), 1)
    sums = jnp.sum(total[...], axis=0, keepdims=True)
    member_of = lax.broadcasted_iota(jnp.int32, (1, rows), 1) // own_tok
    mine = jnp.zeros((1, 128), f32)
    for k in range(n_pop):
        value_k = jnp.sum(jnp.where(member_of == k, sums, 0.0), axis=1, keepdims=True)
        mine = mine + jnp.where(lane_row == k, value_k, 0.0)

    my_id = mc * n_pop + me
    errs[my_id] = mine

    for p, m in others:
        pltpu.make_async_remote_copy(
            src_ref=errs.at[my_id], dst_ref=errs.at[my_id], send_sem=err_send, recv_sem=err_recv,
            device_id={"pop": p, "mp": m}, device_id_type=MESH,
        ).start()
    all_errs = all_of(errs.at[:n_dev - 1], err_send, err_recv)
    for kind in range(len(gathered)):
        packs_done(kind).wait_send()
    all_of(part.at[0], across_send, across_recv.at[0, 0]).wait_send()
    all_of(along_out.at[:levels - 1], along_send, along_recv).wait_send()
    all_of(known.at[:n_pop - 1], known_send, known_recv.at[0]).wait_send()
    all_of(near_in, near_send, near_recv.at[0]).wait_send()
    all_of(far_in, far_send, far_recv.at[0]).wait_send()
    rows_out[0] = pack_q
    rows_out[1] = pack_o
    packs_done(4).wait_recv()
    for i, packs in enumerate((packs_a, packs_b)):
        some = jnp.concatenate([packs[j].astype(f32) for j in range(n_pop)], axis=0)
        some = jnp.concatenate([some] * 3 + [jnp.zeros((left_out.shape[2] - 3 * ranks, cols), f32)], axis=0)
        some = jnp.concatenate(
            [some, jnp.zeros((some.shape[0], left_out.shape[1] - cols), f32)], axis=1
        )
        left_out[i] = some.T.astype(bf16)
    all_errs.wait_recv()
    error = errs[0]
    for i in range(1, n_dev):
        error = error + errs[i]
    live = lane_row < n_pop
    fitness = -(error / (tok * width))
    mean = jnp.sum(jnp.where(live, fitness, 0.0), axis=1, keepdims=True) / n_pop
    dev = jnp.where(live, fitness - mean, 0.0)
    spread = jnp.sum(dev * dev, axis=1, keepdims=True) / n_pop
    weight = dev / jnp.sqrt(spread + spread_floor)
    stat_out[...] = jnp.concatenate(
        [fitness, weight, jnp.zeros((6, 128), f32)], axis=0
    )

    all_errs.wait_send()


def grad_kernel(rows_ref, left_ref, stat_ref, gq_hbm, got_hbm, fit_hbm, gq_ref, got_ref, fit_ref, sem, fit_sem):
    ranks, feats = rows_ref.shape[1:]
    cols = gq_ref.shape[0]
    row = lax.broadcasted_iota(jnp.int32, (ranks, 128), 0)
    lane = lax.broadcasted_iota(jnp.int32, (ranks, 128), 1)
    weight = jnp.sum(jnp.where(lane == row // RANK, stat_ref[1:2, :], 0.0), axis=1, keepdims=True)
    weight = weight / (noise_scale * noise_scale)
    filler = jnp.zeros((left_ref.shape[2] - 3 * ranks, feats), bf16)
    step = cols // (sem.shape[0] // 2)
    copies = []
    for i, (out, target) in enumerate(((gq_ref, gq_hbm), (got_ref, got_hbm))):
        right = jnp.concatenate([*split3(rows_ref[i].astype(f32) * weight), filler], axis=0)
        for low in range(0, cols, step):
            out[low:low + step, :] = dot(left_ref[i, low:low + step, :], right)
            copy = pltpu.make_async_copy(
                out.at[low:low + step], target.at[low:low + step], sem.at[len(copies)]
            )
            copy.start()
            copies.append(copy)
    me = lax.axis_index("pop")
    fit_ref[0] = jnp.sum(jnp.where(lane[:1] == me, stat_ref[0:1, :], 0.0))
    copy = pltpu.make_async_copy(fit_ref, fit_hbm, fit_sem)
    copy.start()
    copies.append(copy)
    for copy in copies:
        copy.wait()


def per_device_fast(
    n_pop, n_mp,
    tokens, target, w_query, w_key, w_value, w_out,
    query_left_factors, query_right_factors, o_left, o_right, member_ids,
):
    tok, width = tokens.shape
    feats = w_query.shape[1]
    cols = w_out.shape[1]
    own_tok = tok // n_pop
    rows = n_pop * own_tok
    cosine, sine = rope_tables(tok, HEAD_DIM)
    half = HEAD_DIM // 2
    by_row = lambda x: np.tile(
        x[:, half:].T.reshape(half, n_pop, own_tok).transpose(1, 0, 2), (1, 1, 128 // own_tok)
    )
    vmem = pl.BlockSpec(memory_space=pltpu.VMEM)
    hbm = pl.BlockSpec(memory_space=pltpu.HBM)
    dma = pltpu.SemaphoreType.DMA
    n_dev = n_pop * n_mp
    like = lambda x: pltpu.VMEM(x.shape, x.dtype)
    wot = w_out.T
    packs, left, stat = pl.pallas_call(
        functools.partial(forward_kernel, n_pop, n_mp, width),
        name="forward",
        out_shape=(
            pltpu.VMEM((2, n_pop * RANK, feats), bf16),
            pltpu.VMEM((2, -(-cols // 128) * 128, n_pop * PACK * 2), bf16),
            pltpu.VMEM((8, 128), f32),
        ),
        in_specs=[hbm] * 15,
        out_specs=(vmem, vmem, vmem),
        scratch_shapes=[
            pltpu.SMEM((1,), jnp.int32), pltpu.VMEM((tok, cols + cols % 128), bf16), pltpu.VMEM((cols + cols % 128, feats), bf16), pltpu.VMEM((RANK, feats), bf16),
            like(tokens), pltpu.VMEM((RANK, width), bf16),
            pltpu.VMEM((RANK, feats), bf16), pltpu.VMEM((RANK, width), bf16),
            pltpu.VMEM((width, 2 * HEAD_DIM), bf16),
            pltpu.VMEM((tok, HEAD_DIM), f32), pltpu.VMEM((tok, HEAD_DIM), f32), like(target),
            pltpu.VMEM((n_pop, HEAD_DIM // 2, 128), f32),
            pltpu.VMEM((n_pop, HEAD_DIM // 2, 128), f32),
            pltpu.VMEM((cols + n_pop * RANK, feats), bf16),
            pltpu.VMEM((2, n_pop // 2, own_tok, feats), LINK),
            pltpu.VMEM((n_pop // 2, own_tok, feats), LINK),
            pltpu.VMEM((n_pop // 2, own_tok, feats), LINK),
            pltpu.VMEM((n_pop // 2, own_tok, feats), LINK),
            pltpu.VMEM((own_tok, feats), f32),
            pltpu.VMEM((n_pop, own_tok, feats), LINK),
            pltpu.VMEM((RANK, tok), bf16),
            pltpu.VMEM((n_pop, RANK, tok), bf16),
            pltpu.VMEM((RANK, feats), bf16),
            pltpu.VMEM((n_pop, RANK, feats), bf16),
            pltpu.VMEM((RANK, feats), bf16),
            pltpu.VMEM((n_pop, RANK, feats), bf16),
            pltpu.VMEM((n_pop, RANK, cols), bf16),
            pltpu.VMEM((n_pop, RANK, cols), bf16),
            pltpu.VMEM((n_pop, RANK, cols), bf16),
            pltpu.VMEM((n_pop, RANK, cols), bf16),
            pltpu.VMEM((n_pop, tok, 2 * HEAD_DIM), bf16),
            pltpu.VMEM((HEAD_DIM + 16, tok), bf16),
            pltpu.VMEM((n_pop, n_pop * RANK, rows), bf16),
            pltpu.VMEM((tok, cols), bf16),
            pltpu.VMEM((2, feats // HEAD_DIM, 2 * HEAD_DIM, rows), bf16),
            pltpu.VMEM((2, feats // HEAD_DIM, tok, rows), f32),
            pltpu.VMEM((2, feats // HEAD_DIM, 8, rows), f32),
            pltpu.VMEM((2, feats // HEAD_DIM, tok, rows), bf16),
            pltpu.VMEM((3, feats, rows), bf16),
            pltpu.VMEM((n_pop, 2, n_mp // 2, cols // n_mp, rows), bf16),
            pltpu.VMEM((n_pop, n_mp // 2, cols // n_mp, rows), bf16),
            pltpu.VMEM((n_pop, cols // n_mp, rows), bf16),
            pltpu.VMEM((n_pop, cols // n_mp, rows), bf16),
            pltpu.VMEM((n_pop, cols // n_mp, rows), f32),
            pltpu.VMEM((8, rows), f32),
            pltpu.VMEM((n_dev, 1, 128), f32),
            dma((16,)), pltpu.SemaphoreType.REGULAR((n_pop // 2 - 1,)),
            dma, dma((n_pop // 2, 2)), dma, dma,
            dma((5,)), dma((5,)), dma, dma((n_pop,)),
            dma, dma((n_pop,)), dma, dma((n_pop,)),
            dma, dma,
        ],
        compiler_params=pltpu.CompilerParams(
            collective_id=0, has_side_effects=True, vmem_limit_bytes=60 * 1024 * 1024
        ),
    )(tokens, w_query, w_key, w_value, wot, target,
      query_left_factors[0].T, query_right_factors[0], o_left[0].T, o_right[0],
      jnp.asarray(cosine), jnp.asarray(sine), jnp.asarray(by_row(cosine)), jnp.asarray(by_row(sine)),
      member_ids)
    grad = jax.ShapeDtypeStruct((cols, feats), f32)
    grad_query, grad_out_t, fitness = pl.pallas_call(
        grad_kernel,
        name="grads",
        out_shape=(grad, grad, jax.ShapeDtypeStruct((1,), f32)),
        in_specs=[vmem, vmem, vmem],
        out_specs=(hbm, hbm, hbm),
        scratch_shapes=[like(grad), like(grad), pltpu.SMEM((1,), f32), dma((8,)), dma],
        compiler_params=pltpu.CompilerParams(vmem_limit_bytes=16 * 1024 * 1024),
    )(packs, left, stat)
    return grad_query, grad_out_t.T, fitness


def tables(count, head_size):
    position = jnp.arange(count, dtype=jnp.float32)
    index = jnp.arange(head_size // 2, dtype=jnp.float32)
    freq = jnp.exp(-math.log(rope_base) * 2.0 * index / head_size)
    angle = position[:, None] * freq[None, :]
    return (jnp.cos(angle)[:, None, :], jnp.sin(angle)[:, None, :])


def rotate(field, cosine_table, sine):
    half = field.shape[-1] // 2
    first = field[..., :half]
    second = field[..., half:]
    return jnp.concatenate(
        [first * cosine_table - second * sine, second * cosine_table + first * sine], axis=-1
    )


def per_device(
    tokens,
    target,
    w_query,
    w_key,
    w_value,
    w_out,
    query_left_factors,
    query_right_factors,
    o_left,
    o_right,
    member_ids,
):
    tok = tokens.shape[0]
    local_feats = w_query.shape[1]
    local_kv = w_key.shape[1] // HEAD_DIM
    group = group_of(w_query, w_key)
    local_heads = local_kv * group
    slots = query_left_factors.shape[0]
    scale = HEAD_DIM ** (-0.5)
    cosine_table, sine = tables(tok, HEAD_DIM)
    base = jnp.dot(
        tokens,
        lax.all_gather(w_query, "pop", axis=0, tiled=True),
        preferred_element_type=jnp.float32,
    )
    keys = rotate(
        jnp.dot(tokens, w_key, preferred_element_type=jnp.float32).reshape(tok, local_kv, HEAD_DIM),
        cosine_table,
        sine,
    ).astype(jnp.bfloat16)
    values = (
        jnp.dot(tokens, w_value, preferred_element_type=jnp.float32)
        .astype(jnp.bfloat16)
        .reshape(tok, local_kv, HEAD_DIM)
    )
    signs = (1 - 2 * (member_ids % 2)).astype(jnp.float32)
    factor = noise_scale * signs[:, None, None]
    lowrank_product = jnp.einsum(
        "td,mdr->mtr", tokens, query_left_factors, preferred_element_type=jnp.float32
    ).astype(jnp.bfloat16)
    query = base[None] + factor * jnp.einsum(
        "olj,ojv->olv", lowrank_product, query_right_factors, preferred_element_type=jnp.float32
    )
    query = rotate(
        query.reshape(slots, tok, local_heads, HEAD_DIM), cosine_table[None], sine[None]
    ).astype(jnp.bfloat16)
    query = query.reshape(slots, tok, local_kv, group, HEAD_DIM)
    scores = jnp.einsum("mtkgd,skd->mkgts", query, keys, preferred_element_type=jnp.float32) * scale
    causal = jnp.arange(tok)[:, None] >= jnp.arange(tok)[None, :]
    scores = jnp.where(causal, scores, -1e30)
    probs = jax.nn.softmax(scores, axis=-1).astype(jnp.bfloat16)
    mixed = (
        jnp.einsum("mkgts,skd->mtkgd", probs, values, preferred_element_type=jnp.float32)
        .astype(jnp.bfloat16)
        .reshape(slots, tok, local_feats)
    )
    low_out = jnp.einsum("mtf,mfr->mtr", mixed, o_left, preferred_element_type=jnp.float32)
    right_full = o_right.astype(jnp.float32)
    part = jnp.einsum(
        "mtf,fe->mte",
        mixed,
        lax.all_gather(w_out, "pop", axis=1, tiled=True),
        preferred_element_type=jnp.float32,
    )
    term = part + factor * jnp.einsum(
        "mtr,mre->mte", low_out, right_full, precision=lax.Precision.HIGHEST
    )
    output = lax.psum_scatter(
        term.astype(jnp.bfloat16), "mp", scatter_dimension=2, tiled=True
    ).astype(jnp.float32)
    diff = output - target.astype(jnp.float32)[None]
    errors = lax.psum(jnp.sum(diff * diff, axis=(1, 2)), "mp")
    fitness = -(errors / (tok * tokens.shape[1]))
    count = slots * lax.axis_size("pop")
    mean = lax.psum(jnp.sum(fitness), "pop") / count
    spread = lax.psum(jnp.sum((fitness - mean) * (fitness - mean)), "pop") / count
    weight = signs * (fitness - mean) / jnp.sqrt(spread + spread_floor)
    every_weight = lax.all_gather(weight, "pop", axis=0, tiled=True)
    right_factors_gathered, left_all = (
        lax.all_gather(query_right_factors, "pop", axis=0, tiled=True),
        lax.all_gather(o_left, "pop", axis=0, tiled=True),
    )
    rows_q = lax.all_to_all(query_left_factors, "pop", split_axis=1, concat_axis=0, tiled=True)
    cols_o = lax.all_to_all(o_right, "pop", split_axis=2, concat_axis=0, tiled=True)
    whole_population = rows_q.shape[0]
    left_q = jnp.transpose(
        rows_q.astype(jnp.float32) * every_weight[:, None, None], (1, 0, 2)
    ).reshape(rows_q.shape[1], whole_population * RANK)
    right_q = right_factors_gathered.astype(jnp.float32).reshape(
        whole_population * RANK, local_feats
    )
    grad_query = jnp.dot(left_q, right_q, precision=lax.Precision.HIGHEST) / noise_scale
    output_left_factor = jnp.transpose(
        left_all.astype(jnp.float32) * every_weight[:, None, None], (1, 0, 2)
    ).reshape(local_feats, whole_population * RANK)
    right_o = cols_o.astype(jnp.float32).reshape(whole_population * RANK, cols_o.shape[2])
    grad_out = jnp.dot(output_left_factor, right_o, precision=lax.Precision.HIGHEST) / noise_scale
    return (grad_query, grad_out, fitness)


def group_of(w_query, w_key):
    return w_query.shape[1] // w_key.shape[1]


def pick(args, n_pop, n_mp):
    tok = args[0].shape[0]
    kernel = (
        args[6].shape[0] == n_pop
        and n_mp == 4
        and n_pop % n_mp == 0
        and n_pop % 2 == 0
        and n_pop * PACK <= 128
        and tok % (n_pop * 16) == 0
        and tok // n_pop < 128
        and 128 % (tok // n_pop) == 0
        and args[5].shape[1] // n_pop % (16 * n_mp) == 0
        and n_pop >= 8
        and n_pop * PACK * 2 % 128 == 0
        and args[2].shape[1] // n_mp == 2 * args[5].shape[1] // n_pop
        and args[2].shape[0] == args[5].shape[1]
        and args[3].shape[1] == n_mp * HEAD_DIM
    )
    return functools.partial(per_device_fast, n_pop, n_mp) if kernel else per_device


def solution(mesh):
    placed = (
        P(),
        P(None, "mp"),
        P("pop", "mp"),
        P(None, "mp"),
        P(None, "mp"),
        P("mp", "pop"),
        P("pop", None, None),
        P("pop", None, "mp"),
        P("pop", "mp", None),
        P("pop", None, None),
        P("pop"),
    )
    n_pop, n_mp = mesh.shape["pop"], mesh.shape["mp"]

    def whole(*args):
        return jax.shard_map(
            pick(args, n_pop, n_mp),
            mesh=mesh,
            in_specs=placed,
            out_specs=(P("pop", "mp"), P("mp", "pop"), P("pop")),
            check_vma=False,
        )(*args)

    return whole
```
